32 devices in a mesh: gx: 8 (over y, x, core), gy: 4 (over z).
Axes of the slice: x: 2, y: 2, z: 4, core: 2. Of those that a mesh axis runs over, the one named last changes fastest.
Arguments:
- right_side: float32 [128, 256, 192], P('gx', 'gy'), may hold values from -46 to 46
- diagonal: float32 [128, 256, 192], P('gx', 'gy'), may hold values from 0.1 to 2
Outputs:
- solution_field: float32 [128, 256, 192], P('gx', 'gy')
- residual: float32 [128, 256, 192], P('gx', 'gy')
The draws below stay inside these ranges and needn't reach their ends.
All inputs are finite; a program needn't handle non-finite values.
Results may differ from the reference program's by a relative error of at most 0.00017.
Values sent between devices are 32-bit elements; how exact they have to be, the bound alone decides.
A program may use at most 64 MiB of HBM per device.

```python
import math
import jax
import jax.numpy as jnp

CZ = 192
ITERS = 3
NX = 128
NY = 256


def draw_right_side(key, part):
    first = jax.random.fold_in(key, 11)
    second = jax.random.fold_in(key, 12)
    ramp = 1.0 + 2.0 * jnp.arange(NX, dtype=jnp.float32) / max(NX - 1, 1)
    ramp = ramp.reshape(NX, 1, 1)
    base = jnp.clip(jax.random.normal(first, (NX, NY, CZ), jnp.float32), -5.0, 5.0)
    column = jnp.exp(jax.random.uniform(second, (NX, NY, 1), jnp.float32) * math.log(3.0))
    return ramp * column * base


def levels(rng, extent, split, least, high):
    gain = 1.0
    for position, parts in split:
        draws = jax.random.uniform(jax.random.fold_in(jax.random.fold_in(rng, 6), position), (parts,), jnp.float32, least / len(split), high / len(split))
        gain = gain * jnp.repeat(jnp.exp(draws), extent[position] // parts).reshape((-1,) + (1,) * (len(extent) - 1 - position))
    return gain


def setup_inputs(seed: int = 0) -> dict:
    arg_keys = jax.random.split(jax.random.key(seed), 3)
    return {
        "right_side": draw_right_side(jax.random.fold_in(arg_keys[2], 71), 0),
        "diagonal": jnp.clip(jnp.exp(math.log(2.0) - 2.9957323 * jax.random.uniform(arg_keys[1], (NX, NY, CZ), jnp.float32) ** levels(arg_keys[1], (NX, NY, CZ), ((0, 8), (1, 4)), -0.2, 0.2)), 0.1, 2.0),
    }


def operate(field, diagonal):
    padded = jnp.pad(field, 1)
    beside = padded[2:, 1:-1, 1:-1] + padded[:-2, 1:-1, 1:-1]
    beside = beside + padded[1:-1, 2:, 1:-1] + padded[1:-1, :-2, 1:-1]
    beside = beside + padded[1:-1, 1:-1, 2:] + padded[1:-1, 1:-1, :-2]
    return (6.0 + diagonal) * field - beside


def reference(right_side, diagonal):
    solution_field = jnp.zeros_like(right_side)
    residual = right_side
    w_field = operate(right_side, diagonal)
    z_field = jnp.zeros_like(right_side)
    s_field = jnp.zeros_like(right_side)
    p_field = jnp.zeros_like(right_side)
    gamma_prev = jnp.float32(1.0)
    alpha_prev = jnp.float32(1.0)
    for step in range(ITERS):
        gamma = jnp.sum(residual * residual)
        delta = jnp.sum(w_field * residual)
        if step == 0:
            beta = jnp.float32(0.0)
            alpha = gamma / delta
        else:
            beta = gamma / gamma_prev
            alpha = gamma / (delta - beta * gamma / alpha_prev)
        s_field = w_field + beta * s_field
        p_field = residual + beta * p_field
        solution_field = solution_field + alpha * p_field
        residual = residual - alpha * s_field
        if step + 1 < ITERS:
            q_field = operate(w_field, diagonal)
            z_field = q_field + beta * z_field
            w_field = w_field - alpha * z_field
        gamma_prev = gamma
        alpha_prev = alpha
    return solution_field, residual
```

```python
import functools

import jax
import jax.numpy as jnp
from jax import lax
from jax.experimental import pallas as pl
from jax.experimental.pallas import tpu as pltpu
from jax.sharding import PartitionSpec as P

ITERS = 3
SHIFT = 7.0
MESH = pl.DeviceIdType.MESH
DIRS = ((1, 0), (-1, 0), (0, 1), (0, -1), (1, 1), (1, -1), (-1, 1), (-1, -1))
RIM = ITERS
ROWS = 8


def span_x(step, width, size):
    if step == 0:
        return pl.ds(0, size), pl.ds(RIM, size)
    if step > 0:
        return pl.ds(size - width, width), pl.ds(RIM - width, width)
    return pl.ds(0, width), pl.ds(RIM + size, width)


def span_y(step, width, size):
    if step == 0:
        return pl.ds(0, size), pl.ds(ROWS, size)
    if step > 0:
        return pl.ds(size - width, width), pl.ds(ROWS - width, width)
    return pl.ds(0, width), pl.ds(ROWS + size, width)


def times_b(field, shift, layer, valid, span=slice(None)):
    here = field[layer, span]
    rows, lanes = here.shape
    row0 = jnp.zeros((1, lanes), jnp.float32)
    lane0 = jnp.zeros((rows, 1), jnp.float32)
    beside = field[layer - 1, span] + field[layer + 1, span]
    beside = beside + jnp.concatenate([here[1:], row0], 0)
    beside = beside + jnp.concatenate([row0, here[:-1]], 0)
    beside = beside + jnp.concatenate([here[:, 1:], lane0], 1)
    beside = beside + jnp.concatenate([lane0, here[:, :-1]], 1)
    out = (shift[layer, span] + (6.0 - SHIFT)) * here - beside
    if valid is None:
        return out
    return jnp.where(valid, out, 0.0)


def coefficients(moments):
    def inner(f, g):
        total = None
        for i, a in enumerate(f):
            for j, c in enumerate(g):
                term = a * c * moments[i + j]
                total = term if total is None else total + term
        return total

    def times_a(f):
        out = [SHIFT * f[0]]
        for k in range(1, len(f)):
            out.append(SHIFT * f[k] + f[k - 1])
        return out + [f[-1]]

    def axpy(f, a, g):
        size = max(len(f), len(g))
        out = []
        for k in range(size):
            if k >= len(f):
                out.append(a * g[k])
            elif k >= len(g):
                out.append(f[k])
            else:
                out.append(f[k] + a * g[k])
        return out

    one = jnp.ones_like(moments[0])
    residual, solution_field = [one], []
    s_field, p_field = [], []
    for step in range(ITERS):
        w_field = times_a(residual)
        gamma = inner(residual, residual)
        delta = inner(w_field, residual)
        if step == 0:
            alpha = gamma / delta
            s_field, p_field = w_field, residual
        else:
            beta = gamma / gamma_prev
            alpha = gamma / (delta - beta * gamma / alpha_prev)
            s_field = axpy(w_field, beta, s_field)
            p_field = axpy(residual, beta, p_field)
        solution_field = axpy(solution_field, alpha, p_field)
        residual = axpy(residual, -alpha, s_field)
        gamma_prev, alpha_prev = gamma, alpha
    return solution_field + residual


def stage_count(nx, ny):
    return (max(nx, ny) - 1).bit_length()


def kernel(nx, ny, b_ref, d_ref, v1_ref, v2_ref, v3_ref, co_ref,
           v0, dd, v1, v2, part, slots,
           tail_out, tail_in, own_sem, send_sem, recv_sem, sum_send, sum_recv, tail_send, tail_recv, ready):
    gx, gy = lax.axis_index("gx"), lax.axis_index("gy")
    bx, by, bz = b_ref.shape
    barrier = pltpu.get_barrier_semaphore()

    def there(dx, dy):
        ok = None
        for at, step, count in ((gx, dx, nx), (gy, dy, ny)):
            if step:
                this = (at + step >= 0) & (at + step < count)
                ok = this if ok is None else ok & this
        return ok

    count = nx * ny
    me = gx * ny + gy

    def peer(k):
        to = lax.rem(me + k, count)
        return to // ny, lax.rem(to, ny)

    own = []
    for n, (src, dst) in enumerate(((b_ref, v0), (d_ref, dd))):
        own.append(pltpu.make_async_copy(
            src, dst.at[pl.ds(RIM, bx), pl.ds(ROWS, by), :], own_sem.at[n]))
        own[-1].start()

    def greet(semaphore, reach):
        for dx, dy in DIRS:
            @pl.when(there(dx * reach, dy * reach))
            def _(dx=dx, dy=dy):
                pl.semaphore_signal(semaphore, inc=1, device_id=(gx + dx * reach, gy + dy * reach),
                                    device_id_type=MESH)

    def greeted(semaphore, reach):
        def span(at, count):
            return 1 + (at >= reach).astype(jnp.int32) + (at + reach < count).astype(jnp.int32)

        pl.semaphore_wait(semaphore, span(gx, nx) * span(gy, ny) - 1)

    greet(barrier, 1)

    @pl.when(gx == 0)
    def _():
        v0[0:RIM] = jnp.zeros((RIM,) + v0.shape[1:], jnp.float32)

    @pl.when(gx == nx - 1)
    def _():
        v0[RIM + bx:] = jnp.zeros((RIM,) + v0.shape[1:], jnp.float32)

    @pl.when(gy == 0)
    def _():
        v0[:, 0:ROWS] = jnp.zeros((v0.shape[0], ROWS, bz), jnp.float32)

    @pl.when(gy == ny - 1)
    def _():
        v0[:, ROWS + by:] = jnp.zeros((v0.shape[0], ROWS, bz), jnp.float32)

    def halo(n, dx, dy):
        width = RIM - n if dx == 0 or dy == 0 else RIM - 1 - n
        width_y = width
        dst = (v0, dd)[n]
        src = dst.at[pl.ds(RIM, bx), pl.ds(ROWS, by), :]
        from_x, to_x = span_x(dx, width, bx)
        from_y, to_y = span_y(dy, width_y, by)
        index = DIRS.index((dx, dy))
        lanes = pl.ds(0, bz // 128 * 128) if dy == 0 else slice(None)
        return pltpu.make_async_remote_copy(
            src_ref=src.at[from_x, from_y, lanes],
            dst_ref=dst.at[to_x, to_y, lanes],
            send_sem=send_sem.at[n, index],
            recv_sem=recv_sem.at[n, index],
            device_id=(gx + dx, gy + dy),
            device_id_type=MESH,
        )

    for copy in own:
        copy.wait()
    full = bz // 128 * 128
    tail = bz - full
    half = by // 2
    last = pl.ds(full, tail)

    def tails(dx, sending):
        first, second = pl.ds(0, tail), pl.ds(tail, tail)
        low = {(True, 1): RIM + bx - 1, (True, -1): RIM, (False, 1): RIM - 1,
               (False, -1): RIM + bx}[sending, dx]
        at = [low - dx * k for k in range(RIM)]
        every = pl.ds(ROWS, by)
        return (
            (v0, at[0], every, pl.ds(0, by), first),
            (v0, at[1], every, pl.ds(0, by), second),
            (v0, at[2], every, pl.ds(by, by), first),
            (dd, at[0], every, pl.ds(by, by), second),
            (dd, at[1], pl.ds(ROWS, half), pl.ds(2 * by, half), first),
            (dd, at[1], pl.ds(ROWS + half, half), pl.ds(2 * by, half), second),
        )

    for side, dx in enumerate((1, -1)):
        for array, layer, rows, to, lanes in tails(dx, True):
            tail_out[side, to, lanes] = array[layer, rows, last]

    def tail_copy(dx):
        side = (1, -1).index(dx)
        return pltpu.make_async_remote_copy(
            src_ref=tail_out.at[side], dst_ref=tail_in.at[side], send_sem=tail_send.at[side],
            recv_sem=tail_recv.at[side], device_id=(gx + dx, gy), device_id_type=MESH)

    def unpack(dx):
        side = (1, -1).index(dx)
        for array, layer, rows, to, lanes in tails(dx, False):
            array[layer, rows, last] = tail_in[side, to, lanes]

    greeted(barrier, 1)

    for n in range(2):
        for dx, dy in DIRS:
            @pl.when(there(dx, dy))
            def _(n=n, dx=dx, dy=dy):
                halo(n, dx, dy).start()

    for dx in (1, -1):
        @pl.when(there(dx, 0))
        def _(dx=dx):
            tail_copy(dx).start()

    stages = stage_count(nx, ny)
    entered = [0]

    def enter():
        if entered[0] > stages:
            return
        if entered[0]:
            greeted(ready.at[entered[0] - 1], 2 ** (entered[0] - 1))
        if entered[0] < stages:
            greet(ready.at[entered[0]], 2 ** entered[0])
        entered[0] += 1

    enter()

    def arrived(directions):
        for n in range(2):
            for dx, dy in directions:
                @pl.when(there(-dx, -dy))
                def _(n=n, dx=dx, dy=dy):
                    halo(n, dx, dy).wait_recv()

    row = lax.broadcasted_iota(jnp.int32, (by + 2 * ROWS, bz), 0)
    inside_y = ((row >= ROWS) | (gy > 0)) & ((row < ROWS + by) | (gy < ny - 1))

    def inside(layer):
        ok = ((layer >= RIM) | (gx > 0)) & ((layer < RIM + bx) | (gx < nx - 1))
        return inside_y & ok

    inner = slice(ROWS, ROWS + by)

    def add_up(layer, span, f3, sums):
        k = layer - RIM
        rows = slice(span.start - ROWS, span.stop - ROWS)
        f0, f1, f2 = v0[layer, span], v1[layer, span], v2[layer, span]
        v1_ref[k, rows] = f1
        v2_ref[k, rows] = f2
        v3_ref[k, rows] = f3
        pairs = (f0 * f0, f0 * f1, f1 * f1, f1 * f2, f2 * f2, f2 * f3)
        groups = (span.stop - span.start) // 8
        return tuple(s + jnp.sum(p.reshape(groups, 8, bz), 0) for s, p in zip(sums, pairs))

    def body(layer, sums):
        return add_up(layer, inner, times_b(v2, dd, layer, None)[inner], sums)

    def stencils(starts, count, valid, sums):
        @pl.loop(0, count[0], unroll=True)
        def _(k):
            layer = starts[0] + k
            v1[layer] = times_b(v0, dd, layer, valid(layer))

        @pl.loop(0, count[1], unroll=True)
        def _(k):
            layer = starts[1] + k
            v2[layer] = times_b(v1, dd, layer, valid(layer))

        return lax.fori_loop(0, count[2], lambda k, s: body(starts[2] + k, s), sums, unroll=True)

    sums = (jnp.zeros((8, bz), jnp.float32),) * 6

    @pl.loop(RIM + 1, RIM + bx - 1, unroll=2)
    def _(layer):
        v1[layer, inner] = times_b(v0, dd, layer, None, inner)

    @pl.loop(RIM + 2, RIM + bx - 2, unroll=2)
    def _(layer):
        v2[layer, inner] = times_b(v1, dd, layer, None, inner)

    middle = slice(2 * ROWS, by)

    def middle_rows(layer, sums):
        f3 = times_b(v2, dd, layer, None, inner)[ROWS:by - ROWS]
        return add_up(layer, middle, f3, sums)

    sums = lax.fori_loop(RIM + 3, RIM + bx - 3, middle_rows, sums, unroll=2)

    enter()
    arrived(DIRS[2:4])
    low_rows, high_rows = slice(0, 3 * ROWS), slice(by - ROWS, by + 2 * ROWS)
    low_in, high_in = gy > 0, gy < ny - 1
    short = lax.broadcasted_iota(jnp.int32, (3 * ROWS, bz), 0)
    low_ok = (short >= ROWS) | low_in
    high_ok = (short < 2 * ROWS) | high_in

    def ends(field, out, layer):
        out[layer, 0:2 * ROWS] = times_b(field, dd, layer, low_ok, low_rows)[:2 * ROWS]
        out[layer, by:by + 2 * ROWS] = times_b(field, dd, layer, high_ok, high_rows)[ROWS:]

    @pl.loop(RIM + 1, RIM + bx - 1, unroll=2)
    def _(layer):
        ends(v0, v1, layer)

    @pl.loop(RIM + 2, RIM + bx - 2, unroll=2)
    def _(layer):
        ends(v1, v2, layer)

    def end_rows(layer, sums):
        f3 = times_b(v2, dd, layer, None, low_rows)[ROWS:2 * ROWS]
        sums = add_up(layer, slice(ROWS, 2 * ROWS), f3, sums)
        f3 = times_b(v2, dd, layer, None, high_rows)[ROWS:2 * ROWS]
        return add_up(layer, slice(by, by + ROWS), f3, sums)

    sums = lax.fori_loop(RIM + 3, RIM + bx - 3, end_rows, sums, unroll=2)
    enter()
    near_high = lax.rem(gx, 2) == 0
    for turn in range(2):
        high = near_high if turn == 0 else jnp.logical_not(near_high)

        @pl.when(high)
        def _():
            arrived([d for d in DIRS if d[0] < 0])

            @pl.when(there(1, 0))
            def _():
                tail_copy(-1).wait_recv()
                unpack(-1)

        @pl.when(jnp.logical_not(high))
        def _():
            arrived([d for d in DIRS if d[0] > 0])

            @pl.when(there(-1, 0))
            def _():
                tail_copy(1).wait_recv()
                unpack(1)

        starts = tuple(jnp.where(high, RIM + bx - 1 - k, RIM - 2 + k) for k in range(3))
        sums = stencils(starts, (3, 3, 3), inside, sums)

    for _ in range(stages):
        enter()
    lane = [jnp.sum(jnp.sum(s, 1, keepdims=True), 0, keepdims=True) for s in sums]
    lane_of = lax.broadcasted_iota(jnp.int32, (1, 128), 1)
    packed = jnp.zeros((1, 128), jnp.float32)
    for k, s in enumerate(lane):
        packed = jnp.where(lane_of == k, s, packed)
    part[0] = packed

    @pl.loop(1, count)
    def _(k):
        pltpu.make_async_remote_copy(
            src_ref=part.at[0], dst_ref=slots.at[me], send_sem=sum_send.at[0],
            recv_sem=sum_recv.at[0], device_id=peer(k), device_id_type=MESH).start()

    slots[me] = packed
    others = slots.at[pl.ds(0, count - 1)]
    pltpu.make_async_copy(others, others, sum_recv.at[0]).wait()
    total = jnp.sum(slots[...], 0)
    moments = [total[:, k:k + 1] for k in range(6)]
    row8 = lax.broadcasted_iota(jnp.int32, (8, 128), 0)
    co = jnp.zeros((8, 128), jnp.float32)
    for k, c in enumerate(coefficients(moments)):
        co = jnp.where(row8 == k, c, co)
    co_ref[...] = co
    pltpu.make_async_copy(others, others, sum_send.at[0]).wait()

    for n in range(2):
        for dx, dy in DIRS:
            @pl.when(there(dx, dy))
            def _(n=n, dx=dx, dy=dy):
                halo(n, dx, dy).wait_send()

    for dx in (1, -1):
        @pl.when(there(dx, 0))
        def _(dx=dx):
            tail_copy(dx).wait_send()


def combine(f0_ref, f1_ref, f2_ref, f3_ref, co_ref, x_ref, r_ref, x_out, r_out, sems):
    c = [co_ref[k:k + 1, 0:1] for k in range(7)]
    count = x_out.shape[0]

    def copy(n, k):
        src, dst = ((x_out, x_ref), (r_out, r_ref))[n]
        return pltpu.make_async_copy(src.at[pl.ds(k, 1)], dst.at[pl.ds(k, 1)], sems.at[n, k])

    @pl.loop(0, count)
    def _(k):
        f0, f1, f2, f3 = f0_ref[k], f1_ref[k], f2_ref[k], f3_ref[k]
        x_out[k] = c[0] * f0 + c[1] * f1 + c[2] * f2
        r_out[k] = c[3] * f0 + c[4] * f1 + c[5] * f2 + c[6] * f3
        for n in range(2):
            copy(n, k).start()

    @pl.loop(0, count)
    def _(k):
        for n in range(2):
            copy(n, k).wait()


def on_device(nx, ny, right_side, diagonal):
    bx, by, bz = right_side.shape
    block = jax.ShapeDtypeStruct((bx, by, bz), jnp.float32)
    big = pltpu.VMEM((bx + 2 * RIM, by + 2 * ROWS, bz), jnp.float32)
    vmem = pl.BlockSpec(memory_space=pltpu.VMEM)
    dma = pltpu.SemaphoreType.DMA
    f1, f2, f3, co = pl.pallas_call(
        functools.partial(kernel, nx, ny),
        out_shape=(block, block, block, jax.ShapeDtypeStruct((8, 128), jnp.float32)),
        in_specs=[pl.BlockSpec(memory_space=pltpu.HBM)] * 2,
        out_specs=(vmem,) * 4,
        scratch_shapes=[
            big, big, big, big,
            pltpu.VMEM((1, 1, 128), jnp.float32),
            pltpu.VMEM((nx * ny, 1, 128), jnp.float32),
            pltpu.VMEM((2, 2 * by + by // 2, 128), jnp.float32),
            pltpu.VMEM((2, 2 * by + by // 2, 128), jnp.float32),
            dma((2,)), dma((2, 8)), dma((2, 8)),
            dma((1,)), dma((1,)), dma((2,)), dma((2,)),
            pltpu.SemaphoreType.REGULAR((stage_count(nx, ny),)),
        ],
        compiler_params=pltpu.CompilerParams(
            collective_id=0, has_side_effects=True, vmem_limit_bytes=24 * 2**20),
    )(*(pltpu.with_memory_space_constraint(a, pltpu.HBM) for a in (right_side, diagonal)))
    return pl.pallas_call(
        combine,
        out_shape=(block, block),
        in_specs=[vmem] * 5,
        out_specs=(pl.BlockSpec(memory_space=pl.ANY),) * 2,
        scratch_shapes=[
            pltpu.VMEM((bx, by, bz), jnp.float32),
            pltpu.VMEM((bx, by, bz), jnp.float32),
            dma((2, bx)),
        ],
        compiler_params=pltpu.CompilerParams(vmem_limit_bytes=24 * 2**20),
    )(right_side, f1, f2, f3, co)


def solution(mesh):
    placed = (P("gx", "gy", None), P("gx", "gy", None))
    return jax.shard_map(
        functools.partial(on_device, mesh.shape["gx"], mesh.shape["gy"]),
        mesh=mesh,
        in_specs=placed,
        out_specs=placed,
        check_vma=False,
    )
```

```python
import functools

import jax
import jax.numpy as jnp
from jax import lax
from jax.experimental import pallas as pl
from jax.experimental.pallas import tpu as pltpu
from jax.sharding import PartitionSpec as P

ITERS = 3
SHIFT = 6.0
MESH = pl.DeviceIdType.MESH
DIRS = ((1, 0), (-1, 0), (0, 1), (0, -1), (1, 1), (1, -1), (-1, 1), (-1, -1))
CORNERS = DIRS[4:]
ROWS = 8
LANES = 128
PIECE = 24


def stage_count(nx, ny):
    return (max(nx, ny) - 1).bit_length()


def coefficients(moments):
    def inner(f, g):
        total = None
        for i, a in enumerate(f):
            for j, c in enumerate(g):
                term = a * c * moments[i + j]
                total = term if total is None else total + term
        return total

    def times_a(f):
        out = [SHIFT * f[0]]
        for k in range(1, len(f)):
            out.append(SHIFT * f[k] + f[k - 1])
        return out + [f[-1]]

    def axpy(f, a, g):
        size = max(len(f), len(g))
        out = []
        for k in range(size):
            if k >= len(f):
                out.append(a * g[k])
            elif k >= len(g):
                out.append(f[k])
            else:
                out.append(f[k] + a * g[k])
        return out

    one = jnp.ones_like(moments[0])
    residual, solution_field = [one], []
    s_field, p_field = [], []
    for step in range(ITERS):
        w_field = times_a(residual)
        gamma = inner(residual, residual)
        delta = inner(w_field, residual)
        if step == 0:
            alpha = gamma / delta
            s_field, p_field = w_field, residual
        else:
            beta = gamma / gamma_prev
            alpha = gamma / (delta - beta * gamma / alpha_prev)
            s_field = axpy(w_field, beta, s_field)
            p_field = axpy(residual, beta, p_field)
        solution_field = axpy(solution_field, alpha, p_field)
        residual = axpy(residual, -alpha, s_field)
        gamma_prev, alpha_prev = gamma, alpha
    return solution_field + residual


def stage_count(nx, ny):
    return (max(nx, ny) - 1).bit_length()


def kernel(nx, ny, b_ref, d_ref, f0m, f0t, v1, v2, v3, co_ref,
           ddm, ddt, fym, fyt, dym, dyt, xs_up, xs_down, xr_low, xr_high, cs, cr, f2r, part, slots,
           own_sem, y_send, y_recv, x_send, x_recv, c_send, c_recv, f_send, f_recv, sum_send, sum_recv, ready):
    gx, gy = lax.axis_index("gx"), lax.axis_index("gy")
    bx, by, bz = b_ref.shape
    tail = bz - LANES
    barrier = pltpu.get_barrier_semaphore()
    own_rows = pl.ds(ROWS, by)
    own_layers = pl.ds(1, bx)
    tall = by + PIECE // 3

    def there(dx, dy):
        ok = None
        for at, step, count in ((gx, dx, nx), (gy, dy, ny)):
            if step:
                this = (at + step >= 0) & (at + step < count)
                ok = this if ok is None else ok & this
        return ok

    count = nx * ny
    me = gx * ny + gy
    low_x, high_x, low_y, high_y = gx > 0, gx < nx - 1, gy > 0, gy < ny - 1

    own = []
    for n, (src, main, end) in enumerate(((b_ref, f0m, f0t), (d_ref, ddm, ddt))):
        for m, (to, lanes) in enumerate(((main, pl.ds(0, LANES)), (end, pl.ds(LANES, tail)))):
            own.append(pltpu.make_async_copy(
                src.at[:, :, lanes], to.at[own_layers, own_rows, :], own_sem.at[2 * n + m]))
            own[-1].start()

    def greet(semaphore, reach):
        for dx, dy in DIRS:
            @pl.when(there(dx * reach, dy * reach))
            def _(dx=dx, dy=dy):
                pl.semaphore_signal(semaphore, inc=1, device_id=(gx + dx * reach, gy + dy * reach),
                                    device_id_type=MESH)

    def greeted(semaphore, reach):
        def span(at, size):
            return 1 + (at >= reach).astype(jnp.int32) + (at + reach < size).astype(jnp.int32)

        pl.semaphore_wait(semaphore, span(gx, nx) * span(gy, ny) - 1)

    greet(barrier, 1)

    def clear(ref):
        ref[...] = jnp.zeros(ref.shape, jnp.float32)

    for k in (0, bx - 2, bx - 1):
        for row in (ROWS - 1, ROWS + by):
            f0m[k + 1, row:row + 1] = jnp.zeros((1, LANES), jnp.float32)
            f0t[k + 1, row:row + 1] = jnp.zeros((1, tail), jnp.float32)
    for side, ok in enumerate((low_y, high_y)):
        @pl.when(jnp.logical_not(ok))
        def _(side=side):
            for ref in (fym, fyt, dym, dyt):
                clear(ref.at[side])
    for ref, ok in ((xr_low, low_x), (xr_high, high_x)):
        @pl.when(jnp.logical_not(ok))
        def _(ref=ref):
            clear(ref)
    for c, (dx, dy) in enumerate(CORNERS):
        @pl.when(jnp.logical_not(there(-dx, -dy)))
        def _(c=c):
            clear(cr.at[c])

    lane = lax.broadcasted_iota(jnp.int32, (PIECE, LANES), 1)
    row = lax.broadcasted_iota(jnp.int32, (PIECE, LANES), 0)

    def rolled(x, by_lanes):
        return pltpu.roll(x, by_lanes, axis=1)

    def widen(x):
        return jnp.concatenate([x, jnp.zeros((x.shape[0], LANES - tail), jnp.float32)], 1)

    def f0(t, layer, start, size):
        rows = pl.ds(start, size)
        return widen(f0t[layer, rows]) if t else f0m[layer, rows]

    def dd(t, layer, start, size):
        rows = pl.ds(start, size)
        return widen(ddt[layer, rows]) if t else ddm[layer, rows]

    def g1(t, layer, start, size):
        return v1[t, layer, pl.ds(start, size)]

    def g2(t, layer, start, size):
        return v2[t, layer, pl.ds(start, size)]

    def beside_z(a, b):
        at = lane[:a.shape[0]]
        left_a, left_b = rolled(a, 1), rolled(b, 1)
        right_a, right_b = rolled(a, LANES - 1), rolled(b, LANES - 1)
        return (jnp.where(at == 0, left_b, left_a) + jnp.where(at == LANES - 1, right_b, right_a),
                jnp.where(at == 0, left_a, left_b) + right_b)

    def times_b(shift, here, others):
        z = beside_z(*here)
        out = []
        for t in range(2):
            total = z[t]
            for o in others:
                total = total + o[t]
            out.append(shift[t] * here[t] - total)
        out[1] = jnp.where(lane[:out[1].shape[0]] < tail, out[1], 0.0)
        return out

    def apply(field, layer, start, size, steps, edges=()):
        two = range(2)
        here = [field(t, layer, start, size) for t in two]
        others = [[field(t, layer, start + step, size) for t in two] for step in (-1, 1)]
        others += [[field(t, layer + step, start, size) for t in two] for step in steps]
        out = times_b([dd(t, layer, start, size) for t in two], here, others)
        if edges:
            at = row + start
            if start < ROWS:
                ok = (at >= ROWS) | low_y
                out = [jnp.where(ok, o, 0.0) for o in out]
            if start + size > ROWS + by:
                ok = (at < ROWS + by) | high_y
                out = [jnp.where(ok, o, 0.0) for o in out]
        return out

    def tall_apply(field, to, layer, first, steps=(-1, 1)):
        for start in range(first, first + tall, PIECE):
            out = apply(field, layer, start, PIECE, steps, True)
            for t in range(2):
                to[t, layer, pl.ds(start, PIECE)] = out[t]

    def halves(a, b):
        return jnp.where(lax.broadcasted_iota(jnp.int32, a.shape, 1) < tail, a, rolled(b, tail))

    for copy in own:
        copy.wait()

    for k, steps, buffer in ((bx - 1, (-1,), xs_up), (0, (1,), xs_down)):
        for start in range(0, by, 16):
            rows = slice(start, start + 16)
            field = [f0(t, k + 1, ROWS + start, 16) for t in range(2)]
            partial = apply(f0, k + 1, ROWS + start, 16, steps)
            buffer[0, rows], buffer[1, rows] = field[0], partial[0]
            buffer[2, rows] = halves(field[1], partial[1])
    for start in range(0, by, 16):
        rows = slice(start, start + 16)
        shift = [dd(t, bx, ROWS + start, 16) for t in range(2)]
        partial = apply(f0, bx - 1, ROWS + start, 16, (-1, 1))
        xs_up[3, rows], xs_up[4, rows] = shift[0], partial[0]
        xs_up[5, rows] = halves(shift[1], partial[1])
    for c, (dx, dy) in enumerate(CORNERS):
        edge, second = (bx, bx - 1) if dx > 0 else (1, 2)
        first, near = (ROWS + by - 2, ROWS + by - 1) if dy > 0 else (ROWS, ROWS)
        cs[c, 0:2] = f0m[edge, first:first + 2]
        cs[c, 2:3] = f0m[second, near:near + 1]
        cs[c, 3:4] = ddm[edge, near:near + 1]
        cs[c, 4:6, 0:tail] = f0t[edge, first:first + 2]
        cs[c, 6:7, 0:tail] = f0t[second, near:near + 1]
        cs[c, 7:8, 0:tail] = ddt[edge, near:near + 1]

    def y_copies(dy):
        side = 0 if dy > 0 else 1
        out = []
        for n, (src, dst, width) in enumerate(((f0m, fym, 3), (f0t, fyt, 3), (ddm, dym, 2), (ddt, dyt, 2))):
            first = ROWS + by - width if dy > 0 else ROWS
            out.append(pltpu.make_async_remote_copy(
                src_ref=src.at[own_layers, pl.ds(first, width), :], dst_ref=dst.at[side],
                send_sem=y_send.at[side, n], recv_sem=y_recv.at[side, n],
                device_id=(gx, gy + dy), device_id_type=MESH))
        return out

    def x_copies(dx):
        if dx > 0:
            pieces = ((xs_up.at[pl.ds(0, 3)], xr_low.at[pl.ds(0, 3)], 0),
                      (xs_up.at[pl.ds(3, 3)], xr_low.at[pl.ds(3, 3)], 1))
        else:
            pieces = ((xs_down, xr_high, 2),)
        return [pltpu.make_async_remote_copy(
            src_ref=src, dst_ref=dst, send_sem=x_send.at[n], recv_sem=x_recv.at[n],
            device_id=(gx + dx, gy), device_id_type=MESH) for src, dst, n in pieces]

    def c_copy(c):
        dx, dy = CORNERS[c]
        return [pltpu.make_async_remote_copy(
            src_ref=cs.at[c], dst_ref=cr.at[c], send_sem=c_send.at[c], recv_sem=c_recv.at[c],
            device_id=(gx + dx, gy + dy), device_id_type=MESH)]

    def f2_copy():
        return [pltpu.make_async_remote_copy(
            src_ref=v2.at[:, 1, own_rows, :], dst_ref=f2r, send_sem=f_send.at[0], recv_sem=f_recv.at[0],
            device_id=(gx - 1, gy), device_id_type=MESH)]

    def every(make, at, what):
        @pl.when(at)
        def _():
            for copy in make():
                getattr(copy, what)()

    x_makes = [(functools.partial(x_copies, dx), (dx, 0)) for dx in (1, -1)]
    y_makes = [(functools.partial(y_copies, dy), (0, dy)) for dy in (1, -1)]
    c_makes = [(functools.partial(c_copy, c), CORNERS[c]) for c in range(4)]

    greeted(barrier, 1)
    for make, (dx, dy) in x_makes + y_makes + c_makes:
        every(make, there(dx, dy), "start")

    def arrived(makes):
        for make, (dx, dy) in makes:
            every(make, there(-dx, -dy), "wait_recv")

    stages = stage_count(nx, ny)
    entered = [0]

    def enter():
        if entered[0] > stages:
            return
        if entered[0]:
            greeted(ready.at[entered[0] - 1], 2 ** (entered[0] - 1))
        if entered[0] < stages:
            greet(ready.at[entered[0]], 2 ** entered[0])
        entered[0] += 1

    enter()

    sums = [jnp.zeros((8, LANES), jnp.float32)] * 6

    def add(n, a, b):
        total = sums[n]
        for t in range(2):
            product = a[t] * b[t]
            for g in range(product.shape[0] // 8):
                total = total + product[8 * g:8 * g + 8]
        sums[n] = total

    def moments(k, which):
        layer = k + 1
        for start in range(ROWS, ROWS + by, 16):
            fields = {}

            def get(n):
                if n not in fields:
                    fields[n] = [(f0, g1, g2)[n](t, layer, start, 16) for t in range(2)]
                return fields[n]

            for n in which:
                if n < 5:
                    add(n, get(n // 2), get((n + 1) // 2))
                else:
                    a, b = get(2)
                    at = lane[:16]
                    left_a, left_b = rolled(a, 1), rolled(b, 1)
                    z = (jnp.where(at == 0, left_b, left_a), jnp.where(at == 0, left_a, left_b))
                    value = []
                    for t in range(2):
                        other = z[t] + g2(t, layer, start - 1, 16) + g2(t, layer - 1, start, 16)
                        value.append(dd(t, layer, start, 16) * get(2)[t] - (other + other))
                    value[1] = jnp.where(at < tail, value[1], 0.0)
                    add(5, get(2), value)

    for k in range(bx):
        moments(k, (0,))
    enter()

    arrived(y_makes)
    enter()
    for ref, small, width in ((f0m, fym, 3), (f0t, fyt, 3), (ddm, dym, 2), (ddt, dyt, 2)):
        ref[1:bx + 1, ROWS - width:ROWS] = small[0]
        ref[1:bx + 1, ROWS + by:ROWS + by + width] = small[1]

    first1, first2 = ROWS - 2, ROWS - 1
    for k in range(bx):
        steps = (1,) if k == 0 else (-1,) if k == bx - 1 else (-1, 1)
        tall_apply(f0, v1, k + 1, first1, steps)
    for k in range(1, bx - 1):
        steps = (1,) if k == 1 else (-1,) if k == bx - 2 else (-1, 1)
        tall_apply(g1, v2, k + 1, first2, steps)
        moments(k, (1, 2))
    for k in range(2, bx - 2):
        moments(k, (3, 4) + ((5,) if k > 2 else ()))

    arrived(x_makes + c_makes)
    for dx in (1, -1):
        got = xr_low if dx > 0 else xr_high
        halo, edge = (0, 1) if dx > 0 else (bx + 1, bx)
        ok = low_x if dx > 0 else high_x
        f0m[halo, ROWS:ROWS + by] = got[0]
        f0t[halo, ROWS:ROWS + by] = got[2][:, :tail]
        corner = [CORNERS.index((dx, dy)) for dy in (1, -1)]
        for c, first in zip(corner, (ROWS - 2, ROWS + by)):
            f0m[halo, first:first + 2] = cr[c, 0:2]
            f0t[halo, first:first + 2] = cr[c, 4:6, 0:tail]
        for start in range(0, by, 16):
            rows = slice(start, start + 16)
            within = (got[1, rows], rolled(got[2, rows], LANES - tail))
            for t in range(2):
                value = within[t] - f0(t, edge, ROWS + start, 16)
                if t:
                    value = jnp.where(lane[:16] < tail, value, 0.0)
                for at, beyond in ((0, -1), (by - 16, 1)):
                    if start == at:
                        where = row[:16] == (0 if beyond < 0 else 15)
                        value = value - jnp.where(where, f0(t, halo, ROWS + start + beyond, 16), 0.0)
                v1[t, halo, pl.ds(ROWS + start, 16)] = jnp.where(ok, value, 0.0)
        for c, at, y_ok in zip(corner, (ROWS - 1, ROWS + by), (low_y, high_y)):
            two = range(2)
            here = [f0(t, halo, at, 1) for t in two]
            others = [[f0(t, halo, at + step, 1) for t in two] for step in (-1, 1)]
            others.append([f0(t, edge, at, 1) for t in two])
            pick = lambda n: [cr[c, n:n + 1], widen(cr[c, n + 4:n + 5, 0:tail])]
            others.append(pick(2))
            out = times_b(pick(3), here, others)
            for t in two:
                v1[t, halo, at:at + 1] = jnp.where(ok & y_ok, out[t], 0.0)
        for start in range(first1, first1 + tall, PIECE):
            for t in range(2):
                v1[t, edge, pl.ds(start, PIECE)] = g1(t, edge, start, PIECE) - f0(t, halo, start, PIECE)
        inner = edge + dx
        tall_apply(g1, v2, edge, first2)
        for start in range(first2, first2 + tall, PIECE):
            for t in range(2):
                v2[t, inner, pl.ds(start, PIECE)] = g2(t, inner, start, PIECE) - g1(t, edge, start, PIECE)
        if dx > 0:
            for start in range(0, by, 16):
                rows, at = slice(start, start + 16), ROWS + start
                two = range(2)
                here = [g1(t, 0, at, 16) for t in two]
                others = [[g1(t, 0, at + step, 16) for t in two] for step in (-1, 1)]
                others.append([g1(t, 1, at, 16) for t in two])
                others.append([got[4, rows], rolled(got[5, rows], LANES - tail)])
                out = times_b([got[3, rows], got[5, rows]], here, others)
                for t in two:
                    value = out[t]
                    for c, where in zip(corner, (0, by - 1)):
                        if start <= where < start + 16:
                            far = widen(cr[c, 6:7, 0:tail]) if t else cr[c, 2:3]
                            value = value + jnp.where(row[:16] == where - start, far, 0.0)
                    v2[t, 0, pl.ds(at, 16)] = jnp.where(low_x, value, 0.0)
            moments(0, (1, 2, 3, 4, 5))
            moments(1, (3, 4, 5))
            moments(2, (5,))
        else:
            moments(bx - 2, (3, 4, 5))
            moments(bx - 1, (1, 2, 3, 4, 5))

    for _ in range(stages):
        enter()
    lane_of = lax.broadcasted_iota(jnp.int32, (8, LANES), 1)
    row_of = lax.broadcasted_iota(jnp.int32, (8, LANES), 0)
    stacked = jnp.zeros((8, LANES), jnp.float32)
    for n, s in enumerate(sums):
        stacked = jnp.where(row_of == n, jnp.sum(s, 0, keepdims=True), stacked)
    packed = jnp.sum(jnp.where(lane_of == row_of, jnp.sum(stacked, 1, keepdims=True), 0.0), 0, keepdims=True)
    part[0] = packed

    def wrapped(at, size):
        return jnp.where(at >= size, at - size, at)

    @pl.loop(0, nx, unroll=nx * ny <= 64)
    def _(i):
        x = wrapped(nx - 1 - gx + i, nx)

        @pl.loop(0, ny, unroll=nx * ny <= 64)
        def _(j):
            y = wrapped(ny - 1 - gy + j, ny)

            @pl.when((x != gx) | (y != gy))
            def _():
                pltpu.make_async_remote_copy(
                    src_ref=part.at[0], dst_ref=slots.at[me], send_sem=sum_send.at[0],
                    recv_sem=sum_recv.at[0], device_id=(x, y), device_id_type=MESH).start()

    every(f2_copy, low_x, "start")
    slots[me] = packed

    for k in range(bx):
        layer = k + 1
        for start in range(ROWS, ROWS + by, 16):
            out = apply(g2, layer, start, 16, (-1, 1) if k < bx - 1 else (-1,))
            for t in range(2):
                v3[t, k, pl.ds(start - ROWS, 16)] = out[t]

    @pl.when(high_x)
    def _():
        for copy in f2_copy():
            copy.wait_recv()
        for t in range(2):
            v3[t, bx - 1] = v3[t, bx - 1] - f2r[t]

    others = slots.at[pl.ds(0, count - 1)]
    pltpu.make_async_copy(others, others, sum_recv.at[0]).wait()
    total = jnp.sum(slots[...], 0)
    moment = [total[:, k:k + 1] for k in range(6)]
    co = jnp.zeros((8, LANES), jnp.float32)
    for k, c in enumerate(coefficients(moment)):
        co = jnp.where(row_of == k, c, co)
    co_ref[...] = co
    pltpu.make_async_copy(others, others, sum_send.at[0]).wait()
    for make, (dx, dy) in x_makes + y_makes + c_makes:
        every(make, there(dx, dy), "wait_send")
    every(f2_copy, low_x, "wait_send")


def combine(f0m, f0t, v1, v2, v3, co_ref, x_out, r_out, x_buf, r_buf, sems):
    bx, by, bz = x_out.shape
    tail = bz - LANES
    c = [jnp.broadcast_to(co_ref[k:k + 1, :], (by, LANES)) for k in range(7)]
    rows = pl.ds(ROWS, by)

    def copy(n, k):
        src, dst = ((x_buf, x_out), (r_buf, r_out))[n]
        return pltpu.make_async_copy(src.at[pl.ds(k, 1)], dst.at[pl.ds(k, 1)], sems.at[n, k])

    for k in range(bx):
        for t in range(2):
            wide = LANES if t == 0 else tail
            lanes = slice(LANES * t, LANES * t + wide)
            f0 = f0t[k + 1, rows] if t else f0m[k + 1, rows]
            f1, f2, f3 = (v1[t, k + 1, rows], v2[t, k + 1, rows], v3[t, k])
            m = [a[:, :wide] for a in c]
            f1, f2, f3 = f1[:, :wide], f2[:, :wide], f3[:, :wide]
            x_buf[k, :, lanes] = m[0] * f0 + m[1] * f1 + m[2] * f2
            r_buf[k, :, lanes] = m[3] * f0 + m[4] * f1 + m[5] * f2 + m[6] * f3
        for n in range(2):
            copy(n, k).start()
    for k in range(bx):
        for n in range(2):
            copy(n, k).wait()


def on_device(nx, ny, right_side, diagonal):
    bx, by, bz = right_side.shape
    tail = bz - LANES
    f32 = jnp.float32
    block = jax.ShapeDtypeStruct((bx, by, bz), f32)
    high, deep = bx + 2, by + 2 * ROWS
    vmem = pl.BlockSpec(memory_space=pltpu.VMEM)
    dma = pltpu.SemaphoreType.DMA
    shape = lambda *dims: jax.ShapeDtypeStruct(dims, f32)
    space = lambda *dims: pltpu.VMEM(dims, f32)
    fields = pl.pallas_call(
        functools.partial(kernel, nx, ny),
        out_shape=(shape(high, deep, LANES), shape(high, deep, tail), shape(2, high, deep, LANES),
                   shape(2, high, deep, LANES), shape(2, bx, by, LANES), shape(8, LANES)),
        in_specs=[pl.BlockSpec(memory_space=pltpu.HBM)] * 2,
        out_specs=(vmem,) * 6,
        scratch_shapes=[
            space(high, deep, LANES), space(high, deep, tail),
            space(2, bx, 3, LANES), space(2, bx, 3, tail), space(2, bx, 2, LANES), space(2, bx, 2, tail),
            space(6, by, LANES), space(3, by, LANES), space(6, by, LANES), space(3, by, LANES),
            space(4, 8, LANES), space(4, 8, LANES), space(2, by, LANES),
            space(1, 1, LANES), space(nx * ny, 1, LANES),
            dma((4,)), dma((2, 4)), dma((2, 4)), dma((3,)), dma((3,)), dma((4,)), dma((4,)),
            dma((1,)), dma((1,)), dma((1,)), dma((1,)),
            pltpu.SemaphoreType.REGULAR((stage_count(nx, ny),)),
        ],
        compiler_params=pltpu.CompilerParams(
            collective_id=0, has_side_effects=True, vmem_limit_bytes=32 * 2**20),
    )(*(pltpu.with_memory_space_constraint(a, pltpu.HBM) for a in (right_side, diagonal)))
    return pl.pallas_call(
        combine,
        out_shape=(block, block),
        in_specs=[vmem] * 6,
        out_specs=(pl.BlockSpec(memory_space=pl.ANY),) * 2,
        scratch_shapes=[space(bx, by, bz), space(bx, by, bz), dma((2, bx))],
        compiler_params=pltpu.CompilerParams(vmem_limit_bytes=24 * 2**20),
    )(*fields)


def solution(mesh):
    placed = (P("gx", "gy", None), P("gx", "gy", None))
    return jax.shard_map(
        functools.partial(on_device, mesh.shape["gx"], mesh.shape["gy"]),
        mesh=mesh,
        in_specs=placed,
        out_specs=placed,
        check_vma=False,
    )
```

```python
import functools

import jax
import jax.numpy as jnp
from jax import lax
from jax.experimental import pallas as pl
from jax.experimental.pallas import tpu as pltpu
from jax.sharding import PartitionSpec as P

SHIFT = 6.0
MESH = pl.DeviceIdType.MESH
DIRS = ((1, 0), (-1, 0), (0, 1), (0, -1), (1, 1), (1, -1), (-1, 1), (-1, -1))
CORNERS = DIRS[4:]
ROWS = 8
LANES = 128
PIECE = 24


def stage_count(nx, ny):
    return (max(nx, ny) - 1).bit_length()


def coefficients(m):
    a = [m[k + 1] + SHIFT * m[k] for k in range(5)]
    inverse0 = 1.0 / a[0]
    lower1, lower2 = a[1] * inverse0, a[2] * inverse0
    inverse1 = 1.0 / (a[2] - a[1] * lower1)
    across = a[3] - a[2] * lower1
    right1, right2 = m[1] - m[0] * lower1, m[2] - m[0] * lower2
    lower3 = across * inverse1
    x2 = (right2 - right1 * lower3) / (a[4] - a[2] * lower2 - across * lower3)
    x1 = (right1 - across * x2) * inverse1
    x0 = (m[0] - a[1] * x1 - a[2] * x2) * inverse0
    return x0, x1, x2, 1.0 - SHIFT * x0, -SHIFT * x1 - x0, -SHIFT * x2 - x1, -x2


def kernel(nx, ny, b_ref, d_ref, f0m, f0t, v1, v2, v3, co_ref,
           ddm, ddt, fym, fyt, dym, dyt, xs_up, xs_down, xr_low, xr_high, cs, cr, f2r, part, slots,
           own_sem, y_send, y_recv, x_send, x_recv, c_send, c_recv, f_send, f_recv, sum_send, sum_recv, ready):
    gx, gy = lax.axis_index("gx"), lax.axis_index("gy")
    bx, by, bz = b_ref.shape
    tail = bz - LANES
    barrier = pltpu.get_barrier_semaphore()
    own_rows = pl.ds(ROWS, by)
    own_layers = pl.ds(1, bx)
    tall = by + PIECE // 3

    def there(dx, dy):
        ok = None
        for at, step, count in ((gx, dx, nx), (gy, dy, ny)):
            if step:
                this = (at + step >= 0) & (at + step < count)
                ok = this if ok is None else ok & this
        return ok

    count = nx * ny
    me = gx * ny + gy
    low_x, high_x, low_y, high_y = gx > 0, gx < nx - 1, gy > 0, gy < ny - 1

    def greet(semaphore, reach):
        for dx, dy in DIRS:
            @pl.when(there(dx * reach, dy * reach))
            def _(dx=dx, dy=dy):
                pl.semaphore_signal(semaphore, inc=1, device_id=(gx + dx * reach, gy + dy * reach),
                                    device_id_type=MESH)

    def greeted(semaphore, reach):
        def span(at, size):
            return 1 + (at >= reach).astype(jnp.int32) + (at + reach < size).astype(jnp.int32)

        pl.semaphore_wait(semaphore, span(gx, nx) * span(gy, ny) - 1)

    greet(barrier, 1)

    own = []
    for n, (src, main, end) in enumerate(((b_ref, f0m, f0t), (d_ref, ddm, ddt))):
        for m, (to, lanes) in enumerate(((main, pl.ds(0, LANES)), (end, pl.ds(LANES, tail)))):
            own.append(pltpu.make_async_copy(
                src.at[:, :, lanes], to.at[own_layers, own_rows, :], own_sem.at[2 * n + m]))
            own[-1].start()

    def clear(ref):
        ref[...] = jnp.zeros(ref.shape, jnp.float32)

    for k in (0, bx - 2, bx - 1):
        for row in (ROWS - 1, ROWS + by):
            f0m[k + 1, row:row + 1] = jnp.zeros((1, LANES), jnp.float32)
            f0t[k + 1, row:row + 1] = jnp.zeros((1, tail), jnp.float32)
    for side, ok in enumerate((low_y, high_y)):
        @pl.when(jnp.logical_not(ok))
        def _(side=side):
            for ref in (fym, fyt, dym, dyt):
                clear(ref.at[side])
    for ref, ok in ((xr_low, low_x), (xr_high, high_x)):
        @pl.when(jnp.logical_not(ok))
        def _(ref=ref):
            clear(ref)
    for c, (dx, dy) in enumerate(CORNERS):
        @pl.when(jnp.logical_not(there(-dx, -dy)))
        def _(c=c):
            clear(cr.at[c])

    lane = lax.broadcasted_iota(jnp.int32, (PIECE, LANES), 1)
    row = lax.broadcasted_iota(jnp.int32, (PIECE, LANES), 0)

    def rolled(x, by_lanes):
        return pltpu.roll(x, by_lanes, axis=1)

    def widen(x):
        return jnp.concatenate([x, jnp.zeros((x.shape[0], LANES - tail), jnp.float32)], 1)

    def f0(t, layer, start, size):
        rows = pl.ds(start, size)
        return widen(f0t[layer, rows]) if t else f0m[layer, rows]

    def dd(t, layer, start, size):
        rows = pl.ds(start, size)
        return widen(ddt[layer, rows]) if t else ddm[layer, rows]

    def g1(t, layer, start, size):
        return v1[t, layer, pl.ds(start, size)]

    def g2(t, layer, start, size):
        return v2[t, layer, pl.ds(start, size)]

    def beside_z(a, b):
        at = lane[:a.shape[0]]
        left_a, left_b = rolled(a, 1), rolled(b, 1)
        right_a, right_b = rolled(a, LANES - 1), rolled(b, LANES - 1)
        return (jnp.where(at == 0, left_b, left_a) + jnp.where(at == LANES - 1, right_b, right_a),
                jnp.where(at == 0, left_a, left_b) + right_b)

    def times_b(shift, here, others):
        z = beside_z(*here)
        out = []
        for t in range(2):
            total = z[t]
            for o in others:
                total = total + o[t]
            out.append(shift[t] * here[t] - total)
        out[1] = jnp.where(lane[:out[1].shape[0]] < tail, out[1], 0.0)
        return out

    def apply(field, layer, start, size, steps, edges=()):
        two = range(2)
        here = [field(t, layer, start, size) for t in two]
        others = [[field(t, layer, start + step, size) for t in two] for step in (-1, 1)]
        others += [[field(t, layer + step, start, size) for t in two] for step in steps]
        out = times_b([dd(t, layer, start, size) for t in two], here, others)
        if edges:
            at = row + start
            if start < ROWS:
                ok = (at >= ROWS) | low_y
                out = [jnp.where(ok, o, 0.0) for o in out]
            if start + size > ROWS + by:
                ok = (at < ROWS + by) | high_y
                out = [jnp.where(ok, o, 0.0) for o in out]
        return out

    def tall_apply(field, to, layer, first, steps=(-1, 1)):
        for start in range(first, first + tall, PIECE):
            out = apply(field, layer, start, PIECE, steps, True)
            for t in range(2):
                to[t, layer, pl.ds(start, PIECE)] = out[t]

    def halves(a, b):
        return jnp.where(lax.broadcasted_iota(jnp.int32, a.shape, 1) < tail, a, rolled(b, tail))

    for copy in own:
        copy.wait()

    for k, steps, buffer in ((bx - 1, (-1,), xs_up), (0, (1,), xs_down)):
        for start in range(0, by, 16):
            rows = slice(start, start + 16)
            field = [f0(t, k + 1, ROWS + start, 16) for t in range(2)]
            partial = apply(f0, k + 1, ROWS + start, 16, steps)
            buffer[0, rows], buffer[1, rows] = field[0], partial[0]
            buffer[2, rows] = halves(field[1], partial[1])
    for start in range(0, by, 16):
        rows = slice(start, start + 16)
        shift = [dd(t, bx, ROWS + start, 16) for t in range(2)]
        partial = apply(f0, bx - 1, ROWS + start, 16, (-1, 1))
        xs_up[3, rows], xs_up[4, rows] = shift[0], partial[0]
        xs_up[5, rows] = halves(shift[1], partial[1])
    for c, (dx, dy) in enumerate(CORNERS):
        edge, second = (bx, bx - 1) if dx > 0 else (1, 2)
        first, near = (ROWS + by - 2, ROWS + by - 1) if dy > 0 else (ROWS, ROWS)
        cs[c, 0:2] = f0m[edge, first:first + 2]
        cs[c, 2:3] = f0m[second, near:near + 1]
        cs[c, 3:4] = ddm[edge, near:near + 1]
        cs[c, 4:6, 0:tail] = f0t[edge, first:first + 2]
        cs[c, 6:7, 0:tail] = f0t[second, near:near + 1]
        cs[c, 7:8, 0:tail] = ddt[edge, near:near + 1]

    def y_copies(dy):
        side = 0 if dy > 0 else 1
        out = []
        for n, (src, dst, width) in enumerate(((f0m, fym, 3), (f0t, fyt, 3), (ddm, dym, 2), (ddt, dyt, 2))):
            first = ROWS + by - width if dy > 0 else ROWS
            out.append(pltpu.make_async_remote_copy(
                src_ref=src.at[own_layers, pl.ds(first, width), :], dst_ref=dst.at[side],
                send_sem=y_send.at[side, n], recv_sem=y_recv.at[side, n],
                device_id=(gx, gy + dy), device_id_type=MESH))
        return out

    def x_copies(dx):
        if dx > 0:
            pieces = ((xs_up.at[pl.ds(0, 3)], xr_low.at[pl.ds(0, 3)], 0),
                      (xs_up.at[pl.ds(3, 3)], xr_low.at[pl.ds(3, 3)], 1))
        else:
            pieces = ((xs_down, xr_high, 2),)
        return [pltpu.make_async_remote_copy(
            src_ref=src, dst_ref=dst, send_sem=x_send.at[n], recv_sem=x_recv.at[n],
            device_id=(gx + dx, gy), device_id_type=MESH) for src, dst, n in pieces]

    def c_copy(c):
        dx, dy = CORNERS[c]
        return [pltpu.make_async_remote_copy(
            src_ref=cs.at[c], dst_ref=cr.at[c], send_sem=c_send.at[c], recv_sem=c_recv.at[c],
            device_id=(gx + dx, gy + dy), device_id_type=MESH)]

    def f2_copy():
        return [pltpu.make_async_remote_copy(
            src_ref=v2.at[:, 1, own_rows, :], dst_ref=f2r, send_sem=f_send.at[0], recv_sem=f_recv.at[0],
            device_id=(gx - 1, gy), device_id_type=MESH)]

    def every(make, at, what):
        @pl.when(at)
        def _():
            for copy in make():
                getattr(copy, what)()

    x_makes = [(functools.partial(x_copies, dx), (dx, 0)) for dx in (1, -1)]
    y_makes = [(functools.partial(y_copies, dy), (0, dy)) for dy in (1, -1)]
    c_makes = [(functools.partial(c_copy, c), CORNERS[c]) for c in range(4)]

    greeted(barrier, 1)
    for make, (dx, dy) in x_makes + y_makes + c_makes:
        every(make, there(dx, dy), "start")

    def arrived(makes):
        for make, (dx, dy) in makes:
            every(make, there(-dx, -dy), "wait_recv")

    stages = stage_count(nx, ny)
    entered = [0]

    def enter():
        if entered[0] > stages:
            return
        if entered[0]:
            greeted(ready.at[entered[0] - 1], 2 ** (entered[0] - 1))
        if entered[0] < stages:
            greet(ready.at[entered[0]], 2 ** entered[0])
        entered[0] += 1

    enter()

    sums = [jnp.zeros((8, LANES), jnp.float32)] * 6

    def add(n, a, b):
        total = sums[n]
        for t in range(2):
            product = a[t] * b[t]
            for g in range(product.shape[0] // 8):
                total = total + product[8 * g:8 * g + 8]
        sums[n] = total

    def moments(k, which):
        layer = k + 1
        for start in range(ROWS, ROWS + by, 16):
            fields = {}

            def get(n):
                if n not in fields:
                    fields[n] = [(f0, g1, g2)[n](t, layer, start, 16) for t in range(2)]
                return fields[n]

            for n in which:
                if n < 5:
                    add(n, get(n // 2), get((n + 1) // 2))
                else:
                    a, b = get(2)
                    at = lane[:16]
                    left_a, left_b = rolled(a, 1), rolled(b, 1)
                    z = (jnp.where(at == 0, left_b, left_a), jnp.where(at == 0, left_a, left_b))
                    value = []
                    for t in range(2):
                        other = z[t] + g2(t, layer, start - 1, 16) + g2(t, layer - 1, start, 16)
                        value.append(dd(t, layer, start, 16) * get(2)[t] - (other + other))
                    value[1] = jnp.where(at < tail, value[1], 0.0)
                    add(5, get(2), value)

    for k in range(bx):
        moments(k, (0,))
    enter()

    arrived(y_makes)
    enter()
    for ref, small, width in ((f0m, fym, 3), (f0t, fyt, 3), (ddm, dym, 2), (ddt, dyt, 2)):
        ref[1:bx + 1, ROWS - width:ROWS] = small[0]
        ref[1:bx + 1, ROWS + by:ROWS + by + width] = small[1]

    first1, first2 = ROWS - 2, ROWS - 1
    for k in range(bx):
        steps = (1,) if k == 0 else (-1,) if k == bx - 1 else (-1, 1)
        tall_apply(f0, v1, k + 1, first1, steps)
    for k in range(1, bx - 1):
        steps = (1,) if k == 1 else (-1,) if k == bx - 2 else (-1, 1)
        tall_apply(g1, v2, k + 1, first2, steps)
        moments(k, (1, 2))
    for k in range(2, bx - 2):
        moments(k, (3, 4) + ((5,) if k > 2 else ()))

    arrived(x_makes + c_makes)
    for dx in (1, -1):
        got = xr_low if dx > 0 else xr_high
        halo, edge = (0, 1) if dx > 0 else (bx + 1, bx)
        ok = low_x if dx > 0 else high_x
        f0m[halo, ROWS:ROWS + by] = got[0]
        f0t[halo, ROWS:ROWS + by] = got[2][:, :tail]
        corner = [CORNERS.index((dx, dy)) for dy in (1, -1)]
        for c, first in zip(corner, (ROWS - 2, ROWS + by)):
            f0m[halo, first:first + 2] = cr[c, 0:2]
            f0t[halo, first:first + 2] = cr[c, 4:6, 0:tail]
        for start in range(0, by, 16):
            rows = slice(start, start + 16)
            within = (got[1, rows], rolled(got[2, rows], LANES - tail))
            for t in range(2):
                value = within[t] - f0(t, edge, ROWS + start, 16)
                if t:
                    value = jnp.where(lane[:16] < tail, value, 0.0)
                for at, beyond in ((0, -1), (by - 16, 1)):
                    if start == at:
                        where = row[:16] == (0 if beyond < 0 else 15)
                        value = value - jnp.where(where, f0(t, halo, ROWS + start + beyond, 16), 0.0)
                v1[t, halo, pl.ds(ROWS + start, 16)] = jnp.where(ok, value, 0.0)
        for c, at, y_ok in zip(corner, (ROWS - 1, ROWS + by), (low_y, high_y)):
            two = range(2)
            here = [f0(t, halo, at, 1) for t in two]
            others = [[f0(t, halo, at + step, 1) for t in two] for step in (-1, 1)]
            others.append([f0(t, edge, at, 1) for t in two])
            pick = lambda n: [cr[c, n:n + 1], widen(cr[c, n + 4:n + 5, 0:tail])]
            others.append(pick(2))
            out = times_b(pick(3), here, others)
            for t in two:
                v1[t, halo, at:at + 1] = jnp.where(ok & y_ok, out[t], 0.0)
        for start in range(first1, first1 + tall, PIECE):
            for t in range(2):
                v1[t, edge, pl.ds(start, PIECE)] = g1(t, edge, start, PIECE) - f0(t, halo, start, PIECE)
        inner = edge + dx
        tall_apply(g1, v2, edge, first2)
        for start in range(first2, first2 + tall, PIECE):
            for t in range(2):
                v2[t, inner, pl.ds(start, PIECE)] = g2(t, inner, start, PIECE) - g1(t, edge, start, PIECE)
        if dx > 0:
            for start in range(0, by, 16):
                rows, at = slice(start, start + 16), ROWS + start
                two = range(2)
                here = [g1(t, 0, at, 16) for t in two]
                others = [[g1(t, 0, at + step, 16) for t in two] for step in (-1, 1)]
                others.append([g1(t, 1, at, 16) for t in two])
                others.append([got[4, rows], rolled(got[5, rows], LANES - tail)])
                out = times_b([got[3, rows], got[5, rows]], here, others)
                for t in two:
                    value = out[t]
                    for c, where in zip(corner, (0, by - 1)):
                        if start <= where < start + 16:
                            far = widen(cr[c, 6:7, 0:tail]) if t else cr[c, 2:3]
                            value = value + jnp.where(row[:16] == where - start, far, 0.0)
                    v2[t, 0, pl.ds(at, 16)] = jnp.where(low_x, value, 0.0)
            moments(0, (1, 2, 3, 4, 5))
            moments(1, (3, 4, 5))
            moments(2, (5,))
        else:
            moments(bx - 2, (3, 4, 5))
            moments(bx - 1, (1, 2, 3, 4, 5))

    for _ in range(stages):
        enter()
    lane_of = lax.broadcasted_iota(jnp.int32, (8, LANES), 1)
    row_of = lax.broadcasted_iota(jnp.int32, (8, LANES), 0)
    stacked = jnp.zeros((8, LANES), jnp.float32)
    for n, s in enumerate(sums):
        stacked = jnp.where(row_of == n, jnp.sum(s, 0, keepdims=True), stacked)
    packed = jnp.sum(jnp.where(lane_of == row_of, jnp.sum(stacked, 1, keepdims=True), 0.0), 0, keepdims=True)
    part[0] = packed

    @pl.loop(0, nx, unroll=nx * ny <= 64)
    def _(x):
        @pl.loop(0, ny, unroll=nx * ny <= 64)
        def _(y):
            @pl.when((x != gx) | (y != gy))
            def _():
                pltpu.make_async_remote_copy(
                    src_ref=part.at[0], dst_ref=slots.at[me], send_sem=sum_send.at[0],
                    recv_sem=sum_recv.at[0], device_id=(x, y), device_id_type=MESH).start()

    every(f2_copy, low_x, "start")
    slots[me] = packed

    for k in range(bx):
        layer = k + 1
        for start in range(ROWS, ROWS + by, 16):
            out = apply(g2, layer, start, 16, (-1, 1) if k < bx - 1 else (-1,))
            for t in range(2):
                v3[t, k, pl.ds(start - ROWS, 16)] = out[t]

    @pl.when(high_x)
    def _():
        for copy in f2_copy():
            copy.wait_recv()
        for t in range(2):
            v3[t, bx - 1] = v3[t, bx - 1] - f2r[t]

    for make, (dx, dy) in x_makes + y_makes + c_makes:
        every(make, there(dx, dy), "wait_send")
    every(f2_copy, low_x, "wait_send")
    others = slots.at[pl.ds(0, count - 1)]
    pltpu.make_async_copy(others, others, sum_send.at[0]).wait()
    pltpu.make_async_copy(others, others, sum_recv.at[0]).wait()
    total = jnp.sum(slots[...], 0)
    moment = [jnp.broadcast_to(total[:, k:k + 1], (1, LANES)) for k in range(6)]
    co = jnp.zeros((8, LANES), jnp.float32)
    for k, c in enumerate(coefficients(moment)):
        co = jnp.where(row_of == k, c, co)
    co_ref[...] = co


def combine(f0m, f0t, v1, v2, v3, co_ref, x_out, r_out, x_buf, r_buf, sems):
    bx, by, bz = x_out.shape
    tail = bz - LANES
    c = [jnp.broadcast_to(co_ref[k:k + 1, :], (by, LANES)) for k in range(7)]
    rows = pl.ds(ROWS, by)

    def copy(n, k):
        src, dst = ((x_buf, x_out), (r_buf, r_out))[n]
        return pltpu.make_async_copy(src.at[pl.ds(k, 1)], dst.at[pl.ds(k, 1)], sems.at[n, k])

    for k in range(bx):
        for t in range(2):
            wide = LANES if t == 0 else tail
            lanes = slice(LANES * t, LANES * t + wide)
            f0 = f0t[k + 1, rows] if t else f0m[k + 1, rows]
            f1, f2, f3 = (v1[t, k + 1, rows], v2[t, k + 1, rows], v3[t, k])
            m = [a[:, :wide] for a in c]
            f1, f2, f3 = f1[:, :wide], f2[:, :wide], f3[:, :wide]
            x_buf[k, :, lanes] = m[0] * f0 + m[1] * f1 + m[2] * f2
            r_buf[k, :, lanes] = m[3] * f0 + m[4] * f1 + m[5] * f2 + m[6] * f3
        for n in range(2):
            copy(n, k).start()
    for k in range(bx):
        for n in range(2):
            copy(n, k).wait()


def on_device(nx, ny, right_side, diagonal):
    bx, by, bz = right_side.shape
    tail = bz - LANES
    f32 = jnp.float32
    block = jax.ShapeDtypeStruct((bx, by, bz), f32)
    high, deep = bx + 2, by + 2 * ROWS
    vmem = pl.BlockSpec(memory_space=pltpu.VMEM)
    dma = pltpu.SemaphoreType.DMA
    shape = lambda *dims: jax.ShapeDtypeStruct(dims, f32)
    space = lambda *dims: pltpu.VMEM(dims, f32)
    fields = pl.pallas_call(
        functools.partial(kernel, nx, ny),
        out_shape=(shape(high, deep, LANES), shape(high, deep, tail), shape(2, high, deep, LANES),
                   shape(2, high, deep, LANES), shape(2, bx, by, LANES), shape(8, LANES)),
        in_specs=[pl.BlockSpec(memory_space=pltpu.HBM)] * 2,
        out_specs=(vmem,) * 6,
        scratch_shapes=[
            space(high, deep, LANES), space(high, deep, tail),
            space(2, bx, 3, LANES), space(2, bx, 3, tail), space(2, bx, 2, LANES), space(2, bx, 2, tail),
            space(6, by, LANES), space(3, by, LANES), space(6, by, LANES), space(3, by, LANES),
            space(4, 8, LANES), space(4, 8, LANES), space(2, by, LANES),
            space(1, 1, LANES), space(nx * ny, 1, LANES),
            dma((4,)), dma((2, 4)), dma((2, 4)), dma((3,)), dma((3,)), dma((4,)), dma((4,)),
            dma((1,)), dma((1,)), dma((1,)), dma((1,)),
            pltpu.SemaphoreType.REGULAR((stage_count(nx, ny),)),
        ],
        compiler_params=pltpu.CompilerParams(
            collective_id=0, has_side_effects=True, vmem_limit_bytes=32 * 2**20),
    )(*(pltpu.with_memory_space_constraint(a, pltpu.HBM) for a in (right_side, diagonal)))
    return pl.pallas_call(
        combine,
        out_shape=(block, block),
        in_specs=[vmem] * 6,
        out_specs=(pl.BlockSpec(memory_space=pl.ANY),) * 2,
        scratch_shapes=[space(bx, by, bz), space(bx, by, bz), dma((2, bx))],
        compiler_params=pltpu.CompilerParams(vmem_limit_bytes=24 * 2**20),
    )(*fields)


def solution(mesh):
    placed = (P("gx", "gy", None), P("gx", "gy", None))
    return jax.shard_map(
        functools.partial(on_device, mesh.shape["gx"], mesh.shape["gy"]),
        mesh=mesh,
        in_specs=placed,
        out_specs=placed,
        check_vma=False,
    )
```

```python
import functools

import jax
import jax.numpy as jnp
from jax import lax
from jax.experimental import pallas as pl
from jax.experimental.pallas import tpu as pltpu
from jax.sharding import PartitionSpec as P

SHIFT = 6.0
MESH = pl.DeviceIdType.MESH
DIRS = ((1, 0), (-1, 0), (0, 1), (0, -1), (1, 1), (1, -1), (-1, 1), (-1, -1))
CORNERS = ((1, 1), (-1, -1), (1, -1), (-1, 1))
ROWS = 8
LANES = 128
CHUNK = 16


def relay_reaches(ny):
    return [2 ** n for n in range((ny - 1).bit_length())]


def coefficients(m):
    a = [m[k + 1] + SHIFT * m[k] for k in range(5)]
    inverse0 = 1.0 / a[0]
    lower1, lower2 = a[1] * inverse0, a[2] * inverse0
    inverse1 = 1.0 / (a[2] - a[1] * lower1)
    across = a[3] - a[2] * lower1
    right1, right2 = m[1] - m[0] * lower1, m[2] - m[0] * lower2
    lower3 = across * inverse1
    x2 = (right2 - right1 * lower3) / (a[4] - a[2] * lower2 - across * lower3)
    x1 = (right1 - across * x2) * inverse1
    x0 = (m[0] - a[1] * x1 - a[2] * x2) * inverse0
    return x0, x1, x2, 1.0 - SHIFT * x0, -SHIFT * x1 - x0, -SHIFT * x2 - x1, -x2


def kernel(nx, ny, b_ref, d_ref, f0m, f0t, v1, v2, v3, co_ref,
           ddm, ddt, xs, xr, ys, yr, cs, cr, ex, ey, hy, fx, fy, fys, fyr, part, slots,
           own_sem, x_send, x_recv, y_send, y_recv, c_send, c_recv,
           fx_send, fx_recv, fy_send, fy_recv, sum_send, sum_recv, ready):
    gx, gy = lax.axis_index("gx"), lax.axis_index("gy")
    bx, by, bz = b_ref.shape
    tail = bz - LANES
    high, deep = f0m.shape[:2]
    two = range(2)
    barrier = pltpu.get_barrier_semaphore()
    count = nx * ny
    me = gx * ny + gy
    x_ok, y_ok = (gx > 0, gx < nx - 1), (gy > 0, gy < ny - 1)
    x_count, y_count = (sum(o.astype(jnp.int32) for o in ok) for ok in (x_ok, y_ok))
    first, last = ROWS, ROWS + by - 1
    x_side = ((0, 1, 2), (bx + 1, bx, bx - 1))
    y_side = ((first - 1, first, first + 1), (last + 1, last, last - 1))
    x_half, y_half = by // 2, bx // 2

    def there(dx, dy):
        ok = None
        for at, step, size in ((gx, dx, nx), (gy, dy, ny)):
            if step:
                this = (at + step >= 0) & (at + step < size)
                ok = this if ok is None else ok & this
        return ok

    def greet(semaphore, reach):
        for dy in (reach, -reach):
            @pl.when(there(0, dy))
            def _(dy=dy):
                pl.semaphore_signal(semaphore, inc=1, device_id=(gx, gy + dy), device_id_type=MESH)

    def greeted(semaphore, reach, more=0):
        present = (gy >= reach).astype(jnp.int32) + (gy + reach < ny).astype(jnp.int32)
        pl.semaphore_wait(semaphore, present + more)

    @pl.loop(0, nx, unroll=nx <= 16)
    def _(x):
        @pl.when(x != gx)
        def _():
            pl.semaphore_signal(barrier, inc=1, device_id=(x, gy), device_id_type=MESH)

    greet(barrier, 1)
    for n, (src, main, end) in enumerate(((b_ref, f0m, f0t), (d_ref, ddm, ddt))):
        for to, lanes in ((main, pl.ds(0, LANES)), (end, pl.ds(LANES, tail))):
            pltpu.make_async_copy(
                src.at[:, :, lanes], to.at[pl.ds(1, bx), pl.ds(ROWS, by), :], own_sem.at[n]).start()

    lane = lax.broadcasted_iota(jnp.int32, (CHUNK, LANES), 1)
    row = lax.broadcasted_iota(jnp.int32, (CHUNK, LANES), 0)

    def zeros(*shape):
        return jnp.zeros(shape, jnp.float32)

    def rolled(x, by_lanes):
        return pltpu.roll(x, by_lanes, axis=1)

    def widen(x):
        return jnp.concatenate([x, zeros(x.shape[0], LANES - tail)], 1)

    def cut(x):
        return jnp.where(lane[:x.shape[0]] < tail, x, 0.0)

    flat_f = (f0m.reshape(high * deep, LANES), f0t.reshape(high * deep, tail))
    flat_d = (ddm.reshape(high * deep, LANES), ddt.reshape(high * deep, tail))
    flat_1 = v1.reshape(2, high * deep, LANES)
    flat_2 = v2.reshape(2, high * deep, LANES)
    flat_3 = v3.reshape(2, bx * by, LANES)

    def along(at, k=0, size=None):
        return pl.ds((k + 1) * deep + at, size or bx, stride=deep)

    def strip_f(t, at):
        return widen(flat_f[1][along(at)]) if t else flat_f[0][along(at)]

    def strip_d(t, at, k=0, size=None):
        rows = along(at, k, size)
        return widen(flat_d[1][rows]) if t else flat_d[0][rows]

    for at in (first - 1, last + 1):
        flat_f[0][along(at)] = zeros(bx, LANES)
        flat_f[1][along(at)] = zeros(bx, tail)
        for t in two:
            flat_1[t, along(at)] = zeros(bx, LANES)
            flat_2[t, along(at)] = zeros(bx, LANES)
            ex[t, at:at + 1] = zeros(1, LANES)
    for side in two:
        @pl.when(jnp.logical_not(x_ok[side]))
        def _(side=side):
            xr[side] = zeros(*xr.shape[1:])
            fx[side] = zeros(*fx.shape[1:])

        @pl.when(jnp.logical_not(y_ok[side]))
        def _(side=side):
            yr[side] = zeros(*yr.shape[1:])
            fyr[side] = zeros(*fyr.shape[1:])
    for c, (dx, dy) in enumerate(CORNERS):
        @pl.when(jnp.logical_not(there(-dx, -dy)))
        def _(c=c):
            cr[c] = zeros(*cr.shape[1:])

    def f0(t, layer, start, size):
        rows = pl.ds(start, size)
        return widen(f0t[layer, rows]) if t else f0m[layer, rows]

    def dd(t, layer, start, size):
        rows = pl.ds(start, size)
        return widen(ddt[layer, rows]) if t else ddm[layer, rows]

    def g1(t, layer, start, size):
        return v1[t, layer, pl.ds(start, size)]

    def g2(t, layer, start, size):
        return v2[t, layer, pl.ds(start, size)]

    def beside_z(a, b):
        at = lane[:a.shape[0]]
        left_a, left_b = rolled(a, 1), rolled(b, 1)
        right_a, right_b = rolled(a, LANES - 1), rolled(b, LANES - 1)
        return (jnp.where(at == 0, left_b, left_a) + jnp.where(at == LANES - 1, right_b, right_a),
                jnp.where(at == 0, left_a, left_b) + right_b)

    def times_b(shift, here, others):
        z = beside_z(*here)
        out = []
        for t in two:
            total = z[t]
            for o in others:
                total = total + o[t]
            out.append(shift[t] * here[t] - total)
        return out[0], cut(out[1])

    def apply(field, layer, start, size, steps):
        def get(layer, start):
            return [field(t, layer, start, size) for t in two]

        others = [get(layer, start - 1), get(layer, start + 1)] + [get(layer + step, start) for step in steps]
        return times_b([dd(t, layer, start, size) for t in two], get(layer, start), others)

    def within(k):
        return (1,) if k == 0 else (-1,) if k == bx - 1 else (-1, 1)

    def pack(buffer, at, main, end):
        size = main.shape[0]
        half = size // 2
        low, up = end[:half], rolled(end[half:], tail)
        buffer[at:at + size] = main
        buffer[at + size:at + size + half] = jnp.where(
            lax.broadcasted_iota(jnp.int32, (half, LANES), 1) < tail, low, up)

    def unpack(buffer, at, size):
        half = size // 2
        both = buffer[at + size:at + size + half]
        keep = lax.broadcasted_iota(jnp.int32, (half, LANES), 1) < tail
        end = [jnp.where(keep, e, 0.0) for e in (both, rolled(both, LANES - tail))]
        return buffer[at:at + size], jnp.concatenate(end, 0)

    part_x, part_y = by * 9 // 4, bx * 9 // 4

    def x_copies(d, piece):
        rows = pl.ds(piece * part_x, part_x)
        return [pltpu.make_async_remote_copy(
            src_ref=xs.at[d, rows], dst_ref=xr.at[d, rows], send_sem=x_send.at[0], recv_sem=x_recv.at[d],
            device_id=(gx + 1 - 2 * d, gy), device_id_type=MESH)]

    def y_copies(d, piece):
        rows = pl.ds(piece * part_y, part_y)
        return [pltpu.make_async_remote_copy(
            src_ref=ys.at[d, rows], dst_ref=yr.at[d, rows], send_sem=y_send.at[0], recv_sem=y_recv.at[0],
            device_id=(gx, gy + 1 - 2 * d), device_id_type=MESH)]

    def start(make, at):
        @pl.when(at)
        def _():
            for copy in make():
                copy.start()

    def wait_all(ref, present, sizes, semaphore):
        for n in sizes:
            @pl.when(present == n)
            def _(n=n):
                some = ref.at[pl.ds(0, n)]
                pltpu.make_async_copy(some, some, semaphore.at[0]).wait()

    for n, ref in enumerate((b_ref, d_ref)):
        pltpu.make_async_copy(ref, ref, own_sem.at[n]).wait()

    for d in two:
        edge = x_side[1 - d][1]
        half = first + d * x_half
        pack(xs.at[d], 0, f0m[edge, first:first + by], widen(f0t[edge, first:first + by]))
        pack(xs.at[d], by * 3 // 2, ddm[edge, half:half + x_half], widen(ddt[edge, half:half + x_half]))
        edge = y_side[1 - d][1]
        pack(ys.at[d], 0, *(strip_f(t, edge) for t in two))
        pack(ys.at[d], bx * 3 // 2, *(strip_d(t, edge, d * y_half, y_half) for t in two))

    greeted(barrier, 1, nx - 1)
    for d in two:
        start(functools.partial(x_copies, d, 0), x_ok[1 - d])
        start(functools.partial(y_copies, d, 0), y_ok[1 - d])

    stages = relay_reaches(ny)
    entered = [0]

    def enter():
        n = entered[0]
        if 0 < n <= len(stages):
            greeted(ready.at[n - 1], stages[n - 1])
        if n < len(stages):
            greet(ready.at[n], stages[n])
        entered[0] += 1

    enter()

    for k in sorted(range(bx), key=lambda k: min(k, bx - 1 - k)):
        for at in range(first, first + by, CHUNK):
            out = apply(f0, k + 1, at, CHUNK, within(k))
            for t in two:
                v1[t, k + 1, pl.ds(at, CHUNK)] = out[t]
    for d in two:
        _, edge, inner = x_side[1 - d]
        half = first + d * x_half
        pack(xs.at[d], part_x, *(v1[t, edge, first:first + by] for t in two))
        pack(xs.at[d], part_x + by * 3 // 2, *(v1[t, inner, half:half + x_half] for t in two))
        _, edge, inner = y_side[1 - d]
        pack(ys.at[d], part_y, *(flat_1[t, along(edge)] for t in two))
        pack(ys.at[d], part_y + bx * 3 // 2, *(flat_1[t, along(inner, d * y_half, y_half)] for t in two))
    for c, (dx, dy) in enumerate(CORNERS):
        _, edge, inner = x_side[dx > 0]
        _, near, next_ = y_side[dy > 0]
        for n, (field, layer, at) in enumerate(
                ((f0, edge, near), (g1, edge, near), (f0, inner, near), (f0, edge, next_))):
            for t in two:
                cs[c, 4 * t + n:4 * t + n + 1] = field(t, layer, at, 1)
    for d in two:
        start(functools.partial(x_copies, d, 1), x_ok[1 - d])
        start(functools.partial(y_copies, d, 1), y_ok[1 - d])
    sums = [zeros(8, LANES)] * 6

    def add(n, a, b):
        total = sums[n]
        for t in two:
            product = a[t] * b[t]
            for g in range(product.shape[0] // 8):
                total = total + product[8 * g:8 * g + 8]
        sums[n] = total

    def moments(k, which, begin, end, size=CHUNK):
        layer = k + 1
        for at in range(first + begin, first + end, size):
            fields = {}

            def get(n):
                if n not in fields:
                    fields[n] = [(f0, g1, g2)[n](t, layer, at, size) for t in two]
                return fields[n]

            for n in which:
                if n < 5:
                    add(n, get(n // 2), get((n + 1) // 2))
                else:
                    a, b = get(2)
                    left_a, left_b = rolled(a, 1), rolled(b, 1)
                    edge = lane[:size] == 0
                    z = (jnp.where(edge, left_b, left_a), jnp.where(edge, left_a, left_b))
                    value = []
                    for t in two:
                        other = z[t] + g2(t, layer, at - 1, size)
                        if k > 2:
                            other = other + g2(t, layer - 1, at, size)
                        value.append(dd(t, layer, at, size) * get(2)[t] - (other + other))
                    add(5, get(2), value)

    for k in range(bx):
        for at in range(first, first + by, CHUNK):
            out = apply(g1, k + 1, at, CHUNK, within(k))
            for t in two:
                v2[t, k + 1, pl.ds(at, CHUNK)] = out[t]
        moments(k, (0,), 0, by)
    enter()
    for c, (dx, dy) in enumerate(CORNERS):
        start(lambda: [pltpu.make_async_remote_copy(
            src_ref=cs.at[c], dst_ref=cr.at[c], send_sem=c_send.at[0], recv_sem=c_recv.at[int(dx < 0)],
            device_id=(gx + dx, gy + dy), device_id_type=MESH)], there(dx, dy))

    def which(k):
        return (1, 2) + ((3, 4, 5) if 1 < k < bx - 2 else ())

    for k in range(1, bx - 1):
        moments(k, which(k), 8, by - 8)

    def corner(c, n):
        return [cr[c, 4 * t + n:4 * t + n + 1] for t in two]

    wait_all(yr, y_count, (1, 2), y_recv)
    for side in two:
        _, edge, inner = y_side[side]
        e, g = unpack(yr.at[side], 0, bx), unpack(yr.at[side], part_y, bx)
        field = [strip_f(t, edge) for t in two]
        f1h = [jnp.where(y_ok[side], g[t] - field[t], 0.0) for t in two]
        shift = lambda x: [jnp.concatenate([zeros(1, LANES), x[:-1]], 0), jnp.concatenate([x[1:], zeros(1, LANES)], 0)]
        moved = [shift(x) for x in e]
        spread = times_b([strip_d(t, edge) for t in two], e, [[m[n] for m in moved] for n in two])
        for t in two:
            flat_1[t, along(edge)] = flat_1[t, along(edge)] - e[t]
            flat_2[t, along(edge)] = flat_2[t, along(edge)] - spread[t] - f1h[t]
            flat_2[t, along(inner)] = flat_2[t, along(inner)] + e[t]
            ey[side, t] = e[t]
            hy[side, t, 1:bx + 1] = f1h[t]
    for begin in (0, by - 8):
        for k in range(1, bx - 1):
            moments(k, which(k), begin, begin + 8, 8)

    def x_phase(turn, carry):
        sums[:] = carry
        odd = lax.rem(gx, 2)
        side = jnp.where(turn == 0, 1 - odd, odd)
        upper = side == 1

        def either(low, up):
            return jnp.where(upper, up, low)

        ok = either(gx, nx - 1 - gx) > 0
        halo, edge, inner, third = (either(n, bx + 1 - n) for n in range(4))
        beyond, near = either(first - 1, last + 1), either(first, last)
        ok_y = either(gy, ny - 1 - gy) > 0

        @pl.when(ok)
        def _():
            pltpu.make_async_copy(xr.at[0], xr.at[0], x_recv.at[side]).wait()
            for n in (1, 2):
                @pl.when(y_count == n)
                def _(n=n):
                    some = cr.at[pl.ds(0, n)]
                    pltpu.make_async_copy(some, some, c_recv.at[side]).wait()

        e, g = unpack(xr.at[side], 0, by), unpack(xr.at[side], part_x, by)
        for t in two:
            ex[t, pl.ds(first, by)] = e[t]
        for at in range(0, by, CHUNK):
            rows = pl.ds(first + at, CHUNK)
            here = [x[at:at + CHUNK] for x in e]
            others = [[ex[t, pl.ds(first + at + step, CHUNK)] for t in two] for step in (-1, 1)]
            spread = times_b([dd(t, edge, first + at, CHUNK) for t in two], here, others)
            for t in two:
                f1h = jnp.where(ok, g[t][at:at + CHUNK] - f0(t, edge, first + at, CHUNK), 0.0)
                v1[t, halo, rows] = f1h
                v1[t, edge, rows] = v1[t, edge, rows] - here[t]
                v2[t, edge, rows] = v2[t, edge, rows] - spread[t] - f1h
                v2[t, inner, rows] = v2[t, inner, rows] + here[t]
        for c, at in ((side, near), (side + 2, first + last - near)):
            for t in two:
                p = corner(c, 0)[t]
                v1[t, halo, pl.ds(at, 1)] = v1[t, halo, pl.ds(at, 1)] - p
                v2[t, edge, pl.ds(at, 1)] = v2[t, edge, pl.ds(at, 1)] + (p + p)
        for t in two:
            value = corner(side, 1)[t] - ey[side, t, pl.ds(edge - 1, 1)] - ex[t, pl.ds(near, 1)]
            value = jnp.where(ok & ok_y, value, 0.0)
            v1[t, halo, pl.ds(beyond, 1)] = value
            hy[side, t, pl.ds(halo, 1)] = value
            hy[side, t, pl.ds(edge, 1)] = hy[side, t, pl.ds(edge, 1)] - corner(side, 0)[t]
        shift = unpack(xr.at[side], by * 3 // 2, x_half)
        far = unpack(xr.at[side], part_x + by * 3 // 2, x_half)
        more = corner(side, 2)
        for at in range(0, x_half, CHUNK):
            begin = first + side * x_half + at
            others = [[g1(t, halo, begin + step, CHUNK) for t in two] for step in (-1, 1)]
            others += [[g1(t, edge, begin, CHUNK) for t in two], [x[at:at + CHUNK] for x in far]]
            out = times_b([x[at:at + CHUNK] for x in shift], [g1(t, halo, begin, CHUNK) for t in two], others)
            value = []
            for t in two:
                o = out[t] + jnp.where(row + begin == near, more[t], 0.0)
                o = jnp.where(ok, o, 0.0)
                fx[side, t, pl.ds(begin - first, CHUNK)] = o
                value.append(o)
            add(5, [-2.0 * g2(t, edge, begin, CHUNK) for t in two], value)
        k = side * y_half
        shift = unpack(yr.at[side], bx * 3 // 2, y_half)
        far = unpack(yr.at[side], part_y + bx * 3 // 2, y_half)
        here, *moved = [[hy[side, t, pl.ds(k + step, y_half)] for t in two] for step in (1, 0, 2)]
        inside = [flat_1[t, along(near, k, y_half)] for t in two]
        out = times_b(shift, here, moved + [inside, far])
        value = []
        for t in two:
            o = out[t] + jnp.where(row[:y_half] + k == edge - 1, corner(side, 3)[t], 0.0)
            o = jnp.where(ok_y, o, 0.0)
            fy[side, t] = o
            value.append(o)
        add(5, [-2.0 * flat_2[t, along(near, k, y_half)] for t in two], value)

        for at in range(first, first + by, CHUNK):
            zero, one, two_e, two_i = (
                [field(t, layer, at, CHUNK) for t in two]
                for field, layer in ((f0, edge), (g1, edge), (g2, edge), (g2, inner)))
            one_i, two_t = ([field(t, layer, at, CHUNK) for t in two] for field, layer in ((g1, inner), (g2, third)))
            add(1, zero, one)
            add(2, one, one)
            for layer, f1_, f2_, next_ in ((edge, one, two_e, two_i), (inner, one_i, two_i, two_t)):
                add(3, f1_, f2_)
                add(4, f2_, f2_)
                left_a, left_b = rolled(f2_[0], 1), rolled(f2_[1], 1)
                z = (jnp.where(lane == 0, left_b, left_a), jnp.where(lane == 0, left_a, left_b))
                value = []
                for t in two:
                    other = z[t] + g2(t, layer, at - 1, CHUNK) + next_[t]
                    value.append(dd(t, layer, at, CHUNK) * f2_[t] - (other + other))
                add(5, f2_, value)
        return tuple(sums)

    sums[:] = lax.fori_loop(0, 2, x_phase, tuple(sums))

    while entered[0] <= len(stages):
        enter()
    lane_of = lane[:8]
    row_of = row[:8]
    stacked = zeros(8, LANES)
    for n, s in enumerate(sums):
        stacked = jnp.where(row_of == n, jnp.sum(s, 0, keepdims=True), stacked)
    packed = jnp.sum(jnp.where(lane_of == row_of, jnp.sum(stacked, 1, keepdims=True), 0.0), 0, keepdims=True)
    part[...] = packed

    @pl.loop(0, nx, unroll=nx * ny <= 64)
    def _(x):
        @pl.loop(0, ny, unroll=nx * ny <= 64)
        def _(y):
            @pl.when((x != gx) | (y != gy))
            def _():
                pltpu.make_async_remote_copy(
                    src_ref=part, dst_ref=slots.at[pl.ds(me, 1)], send_sem=sum_send.at[0],
                    recv_sem=sum_recv.at[0], device_id=(x, y), device_id_type=MESH).start()

    slots[pl.ds(me, 1)] = packed
    for d in two:
        _, edge, _ = x_side[1 - d]
        rows = pl.ds((1 - d) * x_half, x_half)
        start(lambda: [pltpu.make_async_remote_copy(
            src_ref=v2.at[:, edge, pl.ds(first + (1 - d) * x_half, x_half)], dst_ref=fx.at[d, :, rows],
            send_sem=fx_send.at[0], recv_sem=fx_recv.at[0],
            device_id=(gx + 1 - 2 * d, gy), device_id_type=MESH)], x_ok[1 - d])
        _, edge, _ = y_side[1 - d]
        for t in two:
            fys[d, t] = flat_2[t, along(edge, (1 - d) * y_half, y_half)]
        start(lambda: [pltpu.make_async_remote_copy(
            src_ref=fys.at[d], dst_ref=fyr.at[d], send_sem=fy_send.at[0], recv_sem=fy_recv.at[0],
            device_id=(gx, gy + 1 - 2 * d), device_id_type=MESH)], y_ok[1 - d])

    for k in range(bx):
        for at in range(first, first + by, CHUNK):
            out = apply(g2, k + 1, at, CHUNK, within(k))
            for t in two:
                v3[t, k, pl.ds(at - first, CHUNK)] = out[t]

    wait_all(xs, x_count, (1, 2), x_send)
    wait_all(ys, y_count, (1, 2), y_send)
    wait_all(cs, x_count * y_count, (1, 2, 4), c_send)
    half_x, half_y = fx.at[:, :, pl.ds(0, x_half)], fys
    wait_all(half_x, x_count, (1, 2), fx_send)
    wait_all(half_y, y_count, (1, 2), fy_send)
    others = slots.at[pl.ds(0, count - 1)]
    pltpu.make_async_copy(others, others, sum_send.at[0]).wait()
    wait_all(half_x, x_count, (1, 2), fx_recv)
    wait_all(half_y, y_count, (1, 2), fy_recv)
    for side in two:
        edge = x_side[side][1] - 1
        for t in two:
            v3[t, edge] = v3[t, edge] - fx[side, t]
        edge = y_side[side][1] - first
        for t in two:
            pieces = [fy[side, t], fyr[side, t]]
            rows = pl.ds(edge, bx, stride=by)
            flat_3[t, rows] = flat_3[t, rows] - jnp.concatenate(pieces[::-1] if side else pieces, 0)

    pltpu.make_async_copy(others, others, sum_recv.at[0]).wait()
    total = jnp.sum(slots[...], 0, keepdims=True)
    moment = [jnp.broadcast_to(total[:, k:k + 1], (1, LANES)) for k in range(6)]
    co = zeros(8, LANES)
    for k, c in enumerate(coefficients(moment)):
        co = jnp.where(row_of == k, c, co)
    co_ref[...] = co


def combine(f0m, f0t, v1, v2, v3, co_ref, x_out, r_out, x_buf, r_buf, sems):
    bx, by, bz = x_out.shape
    tail = bz - LANES
    c = [jnp.broadcast_to(co_ref[k:k + 1, :], (by, LANES)) for k in range(7)]
    rows = pl.ds(ROWS, by)

    def copy(n, k):
        src, dst = ((x_buf, x_out), (r_buf, r_out))[n]
        return pltpu.make_async_copy(src.at[pl.ds(k, 1)], dst.at[pl.ds(k, 1)], sems.at[n, k])

    for k in range(bx):
        for t in range(2):
            wide = LANES if t == 0 else tail
            lanes = slice(LANES * t, LANES * t + wide)
            f0 = f0t[k + 1, rows] if t else f0m[k + 1, rows]
            f1, f2, f3 = (v1[t, k + 1, rows], v2[t, k + 1, rows], v3[t, k])
            m = [a[:, :wide] for a in c]
            f1, f2, f3 = f1[:, :wide], f2[:, :wide], f3[:, :wide]
            x_buf[k, :, lanes] = m[0] * f0 + m[1] * f1 + m[2] * f2
            r_buf[k, :, lanes] = m[3] * f0 + m[4] * f1 + m[5] * f2 + m[6] * f3
        for n in range(2):
            copy(n, k).start()
    for k in range(bx):
        for n in range(2):
            copy(n, k).wait()


def on_device(nx, ny, right_side, diagonal):
    bx, by, bz = right_side.shape
    tail = bz - LANES
    f32 = jnp.float32
    block = jax.ShapeDtypeStruct((bx, by, bz), f32)
    high, deep = bx + 2, by + 3 * ROWS
    vmem = pl.BlockSpec(memory_space=pltpu.VMEM)
    dma = pltpu.SemaphoreType.DMA
    shape = lambda *dims: jax.ShapeDtypeStruct(dims, f32)
    space = lambda *dims: pltpu.VMEM(dims, f32)
    x_rows, y_rows = by * 9 // 2, bx * 9 // 2
    fields = pl.pallas_call(
        functools.partial(kernel, nx, ny),
        out_shape=(shape(high, deep, LANES), shape(high, deep, tail), shape(2, high, deep, LANES),
                   shape(2, high, deep, LANES), shape(2, bx, by, LANES), shape(8, LANES)),
        in_specs=[pl.BlockSpec(memory_space=pltpu.HBM)] * 2,
        out_specs=(vmem,) * 6,
        scratch_shapes=[
            space(high, deep, LANES), space(high, deep, tail),
            space(2, x_rows, LANES), space(2, x_rows, LANES), space(2, y_rows, LANES), space(2, y_rows, LANES),
            space(4, 8, LANES), space(4, 8, LANES),
            space(2, deep, LANES), space(2, 2, bx, LANES), space(2, 2, bx + 2, LANES),
            space(2, 2, by, LANES), space(2, 2, bx // 2, LANES),
            space(2, 2, bx // 2, LANES), space(2, 2, bx // 2, LANES),
            space(1, LANES), space(nx * ny, LANES),
            dma((2,)), dma((1,)), dma((2,)), dma((1,)), dma((1,)), dma((1,)), dma((2,)), *[dma((1,))] * 6,
            pltpu.SemaphoreType.REGULAR((len(relay_reaches(ny)),)),
        ],
        compiler_params=pltpu.CompilerParams(
            collective_id=0, has_side_effects=True, vmem_limit_bytes=32 * 2**20),
    )(*(pltpu.with_memory_space_constraint(a, pltpu.HBM) for a in (right_side, diagonal)))
    return pl.pallas_call(
        combine,
        out_shape=(block, block),
        in_specs=[vmem] * 6,
        out_specs=(pl.BlockSpec(memory_space=pl.ANY),) * 2,
        scratch_shapes=[space(bx, by, bz), space(bx, by, bz), dma((2, bx))],
        compiler_params=pltpu.CompilerParams(vmem_limit_bytes=24 * 2**20),
    )(*fields)


def solution(mesh):
    placed = (P("gx", "gy", None), P("gx", "gy", None))
    return jax.shard_map(
        functools.partial(on_device, mesh.shape["gx"], mesh.shape["gy"]),
        mesh=mesh,
        in_specs=placed,
        out_specs=placed,
        check_vma=False,
    )
```

```python
import functools

import jax
import jax.numpy as jnp
from jax import lax
from jax.experimental import pallas as pl
from jax.experimental.pallas import tpu as pltpu
from jax.sharding import PartitionSpec as P

SHIFT = 6.0
MESH = pl.DeviceIdType.MESH
DIRS = ((1, 0), (-1, 0), (0, 1), (0, -1), (1, 1), (1, -1), (-1, 1), (-1, -1))
CORNERS = ((1, 1), (-1, -1), (1, -1), (-1, 1))
ROWS = 8
LANES = 128
CHUNK = 16
PIECES = 4
ORDER = (3, 0, 1, 2)


def relay_reaches(ny):
    return [2 ** n for n in range((ny - 1).bit_length())]


def coefficients(m):
    a = [m[k + 1] + SHIFT * m[k] for k in range(5)]
    inverse0 = 1.0 / a[0]
    lower1, lower2 = a[1] * inverse0, a[2] * inverse0
    inverse1 = 1.0 / (a[2] - a[1] * lower1)
    across = a[3] - a[2] * lower1
    right1, right2 = m[1] - m[0] * lower1, m[2] - m[0] * lower2
    lower3 = across * inverse1
    x2 = (right2 - right1 * lower3) / (a[4] - a[2] * lower2 - across * lower3)
    x1 = (right1 - across * x2) * inverse1
    x0 = (m[0] - a[1] * x1 - a[2] * x2) * inverse0
    return x0, x1, x2, 1.0 - SHIFT * x0, -SHIFT * x1 - x0, -SHIFT * x2 - x1, -x2


def kernel(nx, ny, b_ref, d_ref, f0m, f0t, v1, v2, v3, co_ref,
           ddm, ddt, xs, xr, ys, yr, cs, ex, ey, hy, fx, fy, fys, fyr, part, slots,
           own_sem, x_send, x_recv, y_send, y_recv, c_send,
           fx_send, fx_recv, fy_send, fy_recv, sum_send, sum_recv, ready):
    gx, gy = lax.axis_index("gx"), lax.axis_index("gy")
    bx, by, bz = b_ref.shape
    tail = bz - LANES
    high, deep = f0m.shape[:2]
    two = range(2)
    barrier = pltpu.get_barrier_semaphore()
    count = nx * ny
    me = gx * ny + gy
    x_ok, y_ok = (gx > 0, gx < nx - 1), (gy > 0, gy < ny - 1)
    x_count, y_count = (sum(o.astype(jnp.int32) for o in ok) for ok in (x_ok, y_ok))
    first, last = ROWS, ROWS + by - 1
    x_side = ((0, 1, 2), (bx + 1, bx, bx - 1))
    y_side = ((first - 1, first, first + 1), (last + 1, last, last - 1))
    x_half, y_half = by // 2, bx // 2
    part_x, part_y = by * 9 // 4, bx * 9 // 4

    def there(dx, dy):
        ok = None
        for at, step, size in ((gx, dx, nx), (gy, dy, ny)):
            if step:
                this = (at + step >= 0) & (at + step < size)
                ok = this if ok is None else ok & this
        return ok

    def greet(semaphore, reach):
        for dy in (reach, -reach):
            @pl.when(there(0, dy))
            def _(dy=dy):
                pl.semaphore_signal(semaphore, inc=1, device_id=(gx, gy + dy), device_id_type=MESH)

    def greeted(semaphore, reach, more=0):
        present = (gy >= reach).astype(jnp.int32) + (gy + reach < ny).astype(jnp.int32)
        pl.semaphore_wait(semaphore, present + more)

    @pl.loop(0, nx, unroll=nx <= 16)
    def _(x):
        @pl.when(x != gx)
        def _():
            pl.semaphore_signal(barrier, inc=1, device_id=(x, gy), device_id_type=MESH)

    greet(barrier, 1)
    piece = bx // PIECES
    for c in ORDER:
        for src, main, end in ((b_ref, f0m, f0t), (d_ref, ddm, ddt)):
            for to, lanes in ((main, pl.ds(0, LANES)), (end, pl.ds(LANES, tail))):
                pltpu.make_async_copy(
                    src.at[pl.ds(c * piece, piece), :, lanes],
                    to.at[pl.ds(1 + c * piece, piece), pl.ds(ROWS, by), :], own_sem.at[c]).start()

    lane = lax.broadcasted_iota(jnp.int32, (CHUNK, LANES), 1)
    row = lax.broadcasted_iota(jnp.int32, (CHUNK, LANES), 0)

    def zeros(*shape):
        return jnp.zeros(shape, jnp.float32)

    def rolled(x, by_lanes):
        return pltpu.roll(x, by_lanes, axis=1)

    def widen(x):
        return jnp.concatenate([x, zeros(x.shape[0], LANES - tail)], 1)

    def cut(x):
        return jnp.where(lane[:x.shape[0]] < tail, x, 0.0)

    flat_f = (f0m.reshape(high * deep, LANES), f0t.reshape(high * deep, tail))
    flat_d = (ddm.reshape(high * deep, LANES), ddt.reshape(high * deep, tail))
    flat_1 = v1.reshape(2, high * deep, LANES)
    flat_2 = v2.reshape(2, high * deep, LANES)
    flat_3 = v3.reshape(2, bx * by, LANES)

    def along(at, k=0, size=None):
        return pl.ds((k + 1) * deep + at, size or bx, stride=deep)

    def strip_f(t, at):
        return widen(flat_f[1][along(at)]) if t else flat_f[0][along(at)]

    def strip_d(t, at, k=0, size=None):
        rows = along(at, k, size)
        return widen(flat_d[1][rows]) if t else flat_d[0][rows]

    for at in (first - 1, last + 1):
        flat_f[0][along(at)] = zeros(bx, LANES)
        flat_f[1][along(at)] = zeros(bx, tail)
        for t in two:
            flat_1[t, along(at)] = zeros(bx, LANES)
            flat_2[t, along(at)] = zeros(bx, LANES)
            ex[t, at:at + 1] = zeros(1, LANES)
    for side in two:
        @pl.when(jnp.logical_not(x_ok[side]))
        def _(side=side):
            xr[side] = zeros(*xr.shape[1:])
            fx[side] = zeros(*fx.shape[1:])

        @pl.when(jnp.logical_not(y_ok[side]))
        def _(side=side):
            yr[side] = zeros(*yr.shape[1:])
            fyr[side] = zeros(*fyr.shape[1:])
    for c, (dx, dy) in enumerate(CORNERS):
        @pl.when(x_ok[dx < 0] & jnp.logical_not(y_ok[dy < 0]))
        def _(c=c, dx=dx):
            xr[int(dx < 0), pl.ds(part_x * 2 + 8 * (c // 2), 8)] = zeros(8, LANES)

    def f0(t, layer, start, size):
        rows = pl.ds(start, size)
        return widen(f0t[layer, rows]) if t else f0m[layer, rows]

    def dd(t, layer, start, size):
        rows = pl.ds(start, size)
        return widen(ddt[layer, rows]) if t else ddm[layer, rows]

    def g1(t, layer, start, size):
        return v1[t, layer, pl.ds(start, size)]

    def g2(t, layer, start, size):
        return v2[t, layer, pl.ds(start, size)]

    def beside_z(a, b):
        at = lane[:a.shape[0]]
        left_a, left_b = rolled(a, 1), rolled(b, 1)
        right_a, right_b = rolled(a, LANES - 1), rolled(b, LANES - 1)
        return (jnp.where(at == 0, left_b, left_a) + jnp.where(at == LANES - 1, right_b, right_a),
                jnp.where(at == 0, left_a, left_b) + right_b)

    def times_b(shift, here, others):
        z = beside_z(*here)
        out = []
        for t in two:
            total = z[t]
            for o in others:
                total = total + o[t]
            out.append(shift[t] * here[t] - total)
        return out[0], cut(out[1])

    def apply(field, layer, start, size, steps):
        def get(layer, start):
            return [field(t, layer, start, size) for t in two]

        others = [get(layer, start - 1), get(layer, start + 1)] + [get(layer + step, start) for step in steps]
        return times_b([dd(t, layer, start, size) for t in two], get(layer, start), others)

    def within(k):
        return (1,) if k == 0 else (-1,) if k == bx - 1 else (-1, 1)

    def pack(buffer, at, main, end):
        size = main.shape[0]
        half = size // 2
        low, up = end[:half], rolled(end[half:], tail)
        buffer[at:at + size] = main
        buffer[at + size:at + size + half] = jnp.where(
            lax.broadcasted_iota(jnp.int32, (half, LANES), 1) < tail, low, up)

    def unpack(buffer, at, size):
        half = size // 2
        both = buffer[at + size:at + size + half]
        keep = lax.broadcasted_iota(jnp.int32, (half, LANES), 1) < tail
        end = [jnp.where(keep, e, 0.0) for e in (both, rolled(both, LANES - tail))]
        return buffer[at:at + size], jnp.concatenate(end, 0)

    def x_copies(d):
        return [pltpu.make_async_remote_copy(
            src_ref=xs.at[d], dst_ref=xr.at[d, pl.ds(0, part_x * 2)], send_sem=x_send.at[0], recv_sem=x_recv.at[d],
            device_id=(gx + 1 - 2 * d, gy), device_id_type=MESH)]

    def y_copies(d):
        return [pltpu.make_async_remote_copy(
            src_ref=ys.at[d], dst_ref=yr.at[d], send_sem=y_send.at[0], recv_sem=y_recv.at[0],
            device_id=(gx, gy + 1 - 2 * d), device_id_type=MESH)]

    def start(make, at):
        @pl.when(at)
        def _():
            for copy in make():
                copy.start()

    def wait_all(ref, present, sizes, semaphore):
        for n in sizes:
            @pl.when(present == n)
            def _(n=n):
                some = ref.at[pl.ds(0, n)]
                pltpu.make_async_copy(some, some, semaphore.at[0]).wait()

    stages = relay_reaches(ny)
    entered = [0]

    def enter():
        n = entered[0]
        if 0 < n <= len(stages):
            greeted(ready.at[n - 1], stages[n - 1])
        if n < len(stages):
            greet(ready.at[n], stages[n])
        entered[0] += 1

    def come(c):
        some = b_ref.at[pl.ds(0, 2 * piece)]
        pltpu.make_async_copy(some, some, own_sem.at[c]).wait()

    here, done = set(), set()
    for n, c in enumerate(ORDER):
        come(c)
        here |= set(range(c * piece, (c + 1) * piece))
        for k in range(bx):
            if k in done or not {max(k - 1, 0), k, min(k + 1, bx - 1)} <= here:
                continue
            done.add(k)
            for at in range(first, first + by, CHUNK):
                out = apply(f0, k + 1, at, CHUNK, within(k))
                for t in two:
                    v1[t, k + 1, pl.ds(at, CHUNK)] = out[t]
        if n != 1:
            continue
        for d in two:
            _, edge, inner = x_side[1 - d]
            half = first + d * x_half
            pack(xs.at[d], 0, f0m[edge, first:first + by], widen(f0t[edge, first:first + by]))
            pack(xs.at[d], by * 3 // 2, ddm[edge, half:half + x_half], widen(ddt[edge, half:half + x_half]))
            pack(xs.at[d], part_x, *(v1[t, edge, first:first + by] for t in two))
            pack(xs.at[d], part_x + by * 3 // 2, *(v1[t, inner, half:half + x_half] for t in two))
        for c, (dx, dy) in enumerate(CORNERS):
            _, edge, inner = x_side[dx > 0]
            _, near, next_ = y_side[dy > 0]
            for n, (field, layer, at) in enumerate(
                    ((f0, edge, near), (g1, edge, near), (f0, inner, near), (f0, edge, next_))):
                for t in two:
                    cs[c, 4 * t + n:4 * t + n + 1] = field(t, layer, at, 1)
        greeted(barrier, 1, nx - 1)
        for d in two:
            start(functools.partial(x_copies, d), x_ok[1 - d])
        enter()
    for d in two:
        _, edge, inner = y_side[1 - d]
        pack(ys.at[d], 0, *(strip_f(t, edge) for t in two))
        pack(ys.at[d], bx * 3 // 2, *(strip_d(t, edge, d * y_half, y_half) for t in two))
        pack(ys.at[d], part_y, *(flat_1[t, along(edge)] for t in two))
        pack(ys.at[d], part_y + bx * 3 // 2, *(flat_1[t, along(inner, d * y_half, y_half)] for t in two))
        start(functools.partial(y_copies, d), y_ok[1 - d])

    sums = [zeros(8, LANES)] * 6

    def add(n, a, b):
        total = sums[n]
        for t in two:
            product = a[t] * b[t]
            for g in range(product.shape[0] // 8):
                total = total + product[8 * g:8 * g + 8]
        sums[n] = total

    def moments(k, which, begin, end, size=CHUNK):
        layer = k + 1
        for at in range(first + begin, first + end, size):
            fields = {}

            def get(n):
                if n not in fields:
                    fields[n] = [(f0, g1, g2)[n](t, layer, at, size) for t in two]
                return fields[n]

            for n in which:
                if n < 5:
                    add(n, get(n // 2), get((n + 1) // 2))
                else:
                    a, b = get(2)
                    left_a, left_b = rolled(a, 1), rolled(b, 1)
                    edge = lane[:size] == 0
                    z = (jnp.where(edge, left_b, left_a), jnp.where(edge, left_a, left_b))
                    value = []
                    for t in two:
                        other = z[t] + g2(t, layer, at - 1, size)
                        if k > 2:
                            other = other + g2(t, layer - 1, at, size)
                        value.append(dd(t, layer, at, size) * get(2)[t] - (other + other))
                    add(5, get(2), value)

    enter()
    for c, (dx, dy) in enumerate(CORNERS):
        start(lambda: [pltpu.make_async_remote_copy(
            src_ref=cs.at[c], dst_ref=xr.at[int(dx < 0), pl.ds(part_x * 2 + 8 * (c // 2), 8)],
            send_sem=c_send.at[0], recv_sem=x_recv.at[int(dx < 0)],
            device_id=(gx + dx, gy + dy), device_id_type=MESH)], there(dx, dy))
    for k in range(bx):
        for at in range(first, first + by, CHUNK):
            out = apply(g1, k + 1, at, CHUNK, within(k))
            for t in two:
                v2[t, k + 1, pl.ds(at, CHUNK)] = out[t]
        moments(k, (0,), 0, by)
    def which(k):
        return (1, 2) + ((3, 4, 5) if 1 < k < bx - 2 else ())

    for k in range(1, bx - 1):
        moments(k, which(k), 8, by - 8)

    def corner(side, other, n):
        return [xr[side, pl.ds(part_x * 2 + 8 * other + 4 * t + n, 1)] for t in two]

    wait_all(yr, y_count, (1, 2), y_recv)
    for side in two:
        _, edge, inner = y_side[side]
        e, g = unpack(yr.at[side], 0, bx), unpack(yr.at[side], part_y, bx)
        field = [strip_f(t, edge) for t in two]
        f1h = [jnp.where(y_ok[side], g[t] - field[t], 0.0) for t in two]
        shift = lambda x: [jnp.concatenate([zeros(1, LANES), x[:-1]], 0), jnp.concatenate([x[1:], zeros(1, LANES)], 0)]
        moved = [shift(x) for x in e]
        spread = times_b([strip_d(t, edge) for t in two], e, [[m[n] for m in moved] for n in two])
        for t in two:
            flat_1[t, along(edge)] = flat_1[t, along(edge)] - e[t]
            flat_2[t, along(edge)] = flat_2[t, along(edge)] - spread[t] - f1h[t]
            flat_2[t, along(inner)] = flat_2[t, along(inner)] + e[t]
            ey[side, t] = e[t]
            hy[side, t, 1:bx + 1] = f1h[t]
    for begin in (0, by - 8):
        for k in range(1, bx - 1):
            moments(k, which(k), begin, begin + 8, 8)

    def x_phase(turn, carry):
        sums[:] = carry
        odd = lax.rem(gx, 2)
        side = jnp.where(turn == 0, 1 - odd, odd)
        upper = side == 1

        def either(low, up):
            return jnp.where(upper, up, low)

        ok = either(gx, nx - 1 - gx) > 0
        halo, edge, inner, third = (either(n, bx + 1 - n) for n in range(4))
        beyond, near = either(first - 1, last + 1), either(first, last)
        ok_y = either(gy, ny - 1 - gy) > 0

        @pl.when(ok)
        def _():
            for n in (0, 1, 2):
                @pl.when(y_count == n)
                def _(n=n):
                    some = xr.at[0, pl.ds(0, part_x * 2 + 8 * n)]
                    pltpu.make_async_copy(some, some, x_recv.at[side]).wait()

        e, g = unpack(xr.at[side], 0, by), unpack(xr.at[side], part_x, by)
        for t in two:
            ex[t, pl.ds(first, by)] = e[t]
        for at in range(0, by, CHUNK):
            rows = pl.ds(first + at, CHUNK)
            here = [x[at:at + CHUNK] for x in e]
            others = [[ex[t, pl.ds(first + at + step, CHUNK)] for t in two] for step in (-1, 1)]
            spread = times_b([dd(t, edge, first + at, CHUNK) for t in two], here, others)
            for t in two:
                f1h = jnp.where(ok, g[t][at:at + CHUNK] - f0(t, edge, first + at, CHUNK), 0.0)
                v1[t, halo, rows] = f1h
                v1[t, edge, rows] = v1[t, edge, rows] - here[t]
                v2[t, edge, rows] = v2[t, edge, rows] - spread[t] - f1h
                v2[t, inner, rows] = v2[t, inner, rows] + here[t]
        for other, at in ((0, near), (1, first + last - near)):
            for t in two:
                p = corner(side, other, 0)[t]
                v1[t, halo, pl.ds(at, 1)] = v1[t, halo, pl.ds(at, 1)] - p
                v2[t, edge, pl.ds(at, 1)] = v2[t, edge, pl.ds(at, 1)] + (p + p)
        for t in two:
            value = corner(side, 0, 1)[t] - ey[side, t, pl.ds(edge - 1, 1)] - ex[t, pl.ds(near, 1)]
            value = jnp.where(ok & ok_y, value, 0.0)
            v1[t, halo, pl.ds(beyond, 1)] = value
            hy[side, t, pl.ds(halo, 1)] = value
            hy[side, t, pl.ds(edge, 1)] = hy[side, t, pl.ds(edge, 1)] - corner(side, 0, 0)[t]
        shift = unpack(xr.at[side], by * 3 // 2, x_half)
        far = unpack(xr.at[side], part_x + by * 3 // 2, x_half)
        more = corner(side, 0, 2)
        for at in range(0, x_half, CHUNK):
            begin = first + side * x_half + at
            others = [[g1(t, halo, begin + step, CHUNK) for t in two] for step in (-1, 1)]
            others += [[g1(t, edge, begin, CHUNK) for t in two], [x[at:at + CHUNK] for x in far]]
            out = times_b([x[at:at + CHUNK] for x in shift], [g1(t, halo, begin, CHUNK) for t in two], others)
            value = []
            for t in two:
                o = out[t] + jnp.where(row + begin == near, more[t], 0.0)
                o = jnp.where(ok, o, 0.0)
                fx[side, t, pl.ds(begin - first, CHUNK)] = o
                value.append(o)
            add(5, [-2.0 * g2(t, edge, begin, CHUNK) for t in two], value)
        k = side * y_half
        shift = unpack(yr.at[side], bx * 3 // 2, y_half)
        far = unpack(yr.at[side], part_y + bx * 3 // 2, y_half)
        here, *moved = [[hy[side, t, pl.ds(k + step, y_half)] for t in two] for step in (1, 0, 2)]
        inside = [flat_1[t, along(near, k, y_half)] for t in two]
        out = times_b(shift, here, moved + [inside, far])
        value = []
        for t in two:
            o = out[t] + jnp.where(row[:y_half] + k == edge - 1, corner(side, 0, 3)[t], 0.0)
            o = jnp.where(ok_y, o, 0.0)
            fy[side, t] = o
            value.append(o)
        add(5, [-2.0 * flat_2[t, along(near, k, y_half)] for t in two], value)

        for at in range(first, first + by, CHUNK):
            zero, one, two_e, two_i = (
                [field(t, layer, at, CHUNK) for t in two]
                for field, layer in ((f0, edge), (g1, edge), (g2, edge), (g2, inner)))
            one_i, two_t = ([field(t, layer, at, CHUNK) for t in two] for field, layer in ((g1, inner), (g2, third)))
            add(1, zero, one)
            add(2, one, one)
            for layer, f1_, f2_, next_ in ((edge, one, two_e, two_i), (inner, one_i, two_i, two_t)):
                add(3, f1_, f2_)
                add(4, f2_, f2_)
                left_a, left_b = rolled(f2_[0], 1), rolled(f2_[1], 1)
                z = (jnp.where(lane == 0, left_b, left_a), jnp.where(lane == 0, left_a, left_b))
                value = []
                for t in two:
                    other = z[t] + g2(t, layer, at - 1, CHUNK) + next_[t]
                    value.append(dd(t, layer, at, CHUNK) * f2_[t] - (other + other))
                add(5, f2_, value)
        return tuple(sums)

    sums[:] = lax.fori_loop(0, 2, x_phase, tuple(sums))

    while entered[0] <= len(stages):
        enter()
    lane_of = lane[:8]
    row_of = row[:8]
    stacked = zeros(8, LANES)
    for n, s in enumerate(sums):
        stacked = jnp.where(row_of == n, jnp.sum(s, 0, keepdims=True), stacked)
    packed = jnp.sum(jnp.where(lane_of == row_of, jnp.sum(stacked, 1, keepdims=True), 0.0), 0, keepdims=True)
    part[...] = packed

    @pl.loop(0, nx, unroll=nx * ny <= 64)
    def _(x):
        @pl.loop(0, ny, unroll=nx * ny <= 64)
        def _(y):
            @pl.when((x != gx) | (y != gy))
            def _():
                pltpu.make_async_remote_copy(
                    src_ref=part, dst_ref=slots.at[pl.ds(me, 1)], send_sem=sum_send.at[0],
                    recv_sem=sum_recv.at[0], device_id=(x, y), device_id_type=MESH).start()

    slots[pl.ds(me, 1)] = packed
    for d in two:
        _, edge, _ = x_side[1 - d]
        rows = pl.ds((1 - d) * x_half, x_half)
        start(lambda: [pltpu.make_async_remote_copy(
            src_ref=v2.at[:, edge, pl.ds(first + (1 - d) * x_half, x_half)], dst_ref=fx.at[d, :, rows],
            send_sem=fx_send.at[0], recv_sem=fx_recv.at[0],
            device_id=(gx + 1 - 2 * d, gy), device_id_type=MESH)], x_ok[1 - d])
        _, edge, _ = y_side[1 - d]
        for t in two:
            fys[d, t] = flat_2[t, along(edge, (1 - d) * y_half, y_half)]
        start(lambda: [pltpu.make_async_remote_copy(
            src_ref=fys.at[d], dst_ref=fyr.at[d], send_sem=fy_send.at[0], recv_sem=fy_recv.at[0],
            device_id=(gx, gy + 1 - 2 * d), device_id_type=MESH)], y_ok[1 - d])

    for k in range(bx):
        for at in range(first, first + by, CHUNK):
            out = apply(g2, k + 1, at, CHUNK, within(k))
            for t in two:
                v3[t, k, pl.ds(at - first, CHUNK)] = out[t]

    wait_all(xs, x_count, (1, 2), x_send)
    wait_all(ys, y_count, (1, 2), y_send)
    wait_all(cs, x_count * y_count, (1, 2, 4), c_send)
    half_x, half_y = fx.at[:, :, pl.ds(0, x_half)], fys
    wait_all(half_x, x_count, (1, 2), fx_send)
    wait_all(half_y, y_count, (1, 2), fy_send)
    others = slots.at[pl.ds(0, count - 1)]
    pltpu.make_async_copy(others, others, sum_send.at[0]).wait()
    wait_all(half_x, x_count, (1, 2), fx_recv)
    wait_all(half_y, y_count, (1, 2), fy_recv)
    for side in two:
        edge = x_side[side][1] - 1
        for t in two:
            v3[t, edge] = v3[t, edge] - fx[side, t]
        edge = y_side[side][1] - first
        for t in two:
            pieces = [fy[side, t], fyr[side, t]]
            rows = pl.ds(edge, bx, stride=by)
            flat_3[t, rows] = flat_3[t, rows] - jnp.concatenate(pieces[::-1] if side else pieces, 0)

    pltpu.make_async_copy(others, others, sum_recv.at[0]).wait()
    total = jnp.sum(slots[...], 0, keepdims=True)
    moment = [jnp.broadcast_to(total[:, k:k + 1], (1, LANES)) for k in range(6)]
    co = zeros(8, LANES)
    for k, c in enumerate(coefficients(moment)):
        co = jnp.where(row_of == k, c, co)
    co_ref[...] = co


def combine(f0m, f0t, v1, v2, v3, co_ref, x_out, r_out, x_buf, r_buf, sems):
    bx, by, bz = x_out.shape
    tail = bz - LANES
    c = [jnp.broadcast_to(co_ref[k:k + 1, :], (by, LANES)) for k in range(7)]
    rows = pl.ds(ROWS, by)

    def copy(n, k):
        src, dst = ((x_buf, x_out), (r_buf, r_out))[n]
        return pltpu.make_async_copy(src.at[pl.ds(k, 1)], dst.at[pl.ds(k, 1)], sems.at[n])

    for k in range(bx):
        for t in range(2):
            wide = LANES if t == 0 else tail
            lanes = slice(LANES * t, LANES * t + wide)
            f0 = f0t[k + 1, rows] if t else f0m[k + 1, rows]
            f1, f2, f3 = (v1[t, k + 1, rows], v2[t, k + 1, rows], v3[t, k])
            m = [a[:, :wide] for a in c]
            f1, f2, f3 = f1[:, :wide], f2[:, :wide], f3[:, :wide]
            x_buf[k, :, lanes] = m[0] * f0 + m[1] * f1 + m[2] * f2
            r_buf[k, :, lanes] = m[3] * f0 + m[4] * f1 + m[5] * f2 + m[6] * f3
        for n in range(2):
            copy(n, k).start()
    for n, (src, dst) in enumerate(((x_buf, x_out), (r_buf, r_out))):
        pltpu.make_async_copy(src, dst, sems.at[n]).wait()


def on_device(nx, ny, right_side, diagonal):
    bx, by, bz = right_side.shape
    tail = bz - LANES
    f32 = jnp.float32
    block = jax.ShapeDtypeStruct((bx, by, bz), f32)
    high, deep = bx + 2, by + 3 * ROWS
    vmem = pl.BlockSpec(memory_space=pltpu.VMEM)
    dma = pltpu.SemaphoreType.DMA
    shape = lambda *dims: jax.ShapeDtypeStruct(dims, f32)
    space = lambda *dims: pltpu.VMEM(dims, f32)
    x_rows, y_rows = by * 9 // 2, bx * 9 // 2
    fields = pl.pallas_call(
        functools.partial(kernel, nx, ny),
        out_shape=(shape(high, deep, LANES), shape(high, deep, tail), shape(2, high, deep, LANES),
                   shape(2, high, deep, LANES), shape(2, bx, by, LANES), shape(8, LANES)),
        in_specs=[pl.BlockSpec(memory_space=pltpu.HBM)] * 2,
        out_specs=(vmem,) * 6,
        scratch_shapes=[
            space(high, deep, LANES), space(high, deep, tail),
            space(2, x_rows, LANES), space(2, x_rows + 16, LANES), space(2, y_rows, LANES), space(2, y_rows, LANES),
            space(4, 8, LANES),
            space(2, deep, LANES), space(2, 2, bx, LANES), space(2, 2, bx + 2, LANES),
            space(2, 2, by, LANES), space(2, 2, bx // 2, LANES),
            space(2, 2, bx // 2, LANES), space(2, 2, bx // 2, LANES),
            space(1, LANES), space(nx * ny, LANES),
            dma((PIECES,)), dma((1,)), dma((2,)), dma((1,)), dma((1,)), dma((1,)), *[dma((1,))] * 6,
            pltpu.SemaphoreType.REGULAR((len(relay_reaches(ny)),)),
        ],
        compiler_params=pltpu.CompilerParams(
            collective_id=0, has_side_effects=True, vmem_limit_bytes=32 * 2**20),
    )(*(pltpu.with_memory_space_constraint(a, pltpu.HBM) for a in (right_side, diagonal)))
    return pl.pallas_call(
        combine,
        out_shape=(block, block),
        in_specs=[vmem] * 6,
        out_specs=(pl.BlockSpec(memory_space=pl.ANY),) * 2,
        scratch_shapes=[space(bx, by, bz), space(bx, by, bz), dma((2,))],
        compiler_params=pltpu.CompilerParams(vmem_limit_bytes=24 * 2**20),
    )(*fields)


def solution(mesh):
    placed = (P("gx", "gy", None), P("gx", "gy", None))
    return jax.shard_map(
        functools.partial(on_device, mesh.shape["gx"], mesh.shape["gy"]),
        mesh=mesh,
        in_specs=placed,
        out_specs=placed,
        check_vma=False,
    )
```

```python
import functools

import jax
import jax.numpy as jnp
from jax import lax
from jax.experimental import pallas as pl
from jax.experimental.pallas import tpu as pltpu
from jax.sharding import PartitionSpec as P

SHIFT = 6.0
MESH = pl.DeviceIdType.MESH
DIRS = ((1, 0), (-1, 0), (0, 1), (0, -1), (1, 1), (1, -1), (-1, 1), (-1, -1))
CORNERS = ((1, 1), (-1, -1), (1, -1), (-1, 1))
ROWS = 8
LANES = 128
CHUNK = 16
PIECES = 4
ORDER = (3, 0, 1, 2)


def relay_reaches(ny):
    return [2 ** n for n in range((ny - 1).bit_length())]


def coefficients(m):
    a = [m[k + 1] + SHIFT * m[k] for k in range(5)]
    inverse0 = 1.0 / a[0]
    lower1, lower2 = a[1] * inverse0, a[2] * inverse0
    inverse1 = 1.0 / (a[2] - a[1] * lower1)
    across = a[3] - a[2] * lower1
    right1, right2 = m[1] - m[0] * lower1, m[2] - m[0] * lower2
    lower3 = across * inverse1
    x2 = (right2 - right1 * lower3) / (a[4] - a[2] * lower2 - across * lower3)
    x1 = (right1 - across * x2) * inverse1
    x0 = (m[0] - a[1] * x1 - a[2] * x2) * inverse0
    return x0, x1, x2, 1.0 - SHIFT * x0, -SHIFT * x1 - x0, -SHIFT * x2 - x1, -x2


def kernel(nx, ny, b_ref, d_ref, f0m, f0t, v1, v2, v3, co_ref,
           ddm, ddt, xs, xr, ys, yr, cs, ex, ey, hy, fx, fy, fys, fyr, part, slots,
           own_sem, x_send, x_recv, y_send, y_recv, c_send,
           fx_send, fx_recv, fy_send, fy_recv, sum_send, sum_recv, ready):
    gx, gy = lax.axis_index("gx"), lax.axis_index("gy")
    bx, by, bz = b_ref.shape
    tail = bz - LANES
    high, deep = f0m.shape[:2]
    two = range(2)
    barrier = pltpu.get_barrier_semaphore()
    count = nx * ny
    me = gx * ny + gy
    x_ok, y_ok = (gx > 0, gx < nx - 1), (gy > 0, gy < ny - 1)
    x_count, y_count = (sum(o.astype(jnp.int32) for o in ok) for ok in (x_ok, y_ok))
    first, last = ROWS, ROWS + by - 1
    x_side = ((0, 1, 2), (bx + 1, bx, bx - 1))
    y_side = ((first - 1, first, first + 1), (last + 1, last, last - 1))
    x_half, y_half = by // 2, bx // 2
    part_x, part_y = by * 9 // 4, bx * 9 // 4

    def there(dx, dy):
        ok = None
        for at, step, size in ((gx, dx, nx), (gy, dy, ny)):
            if step:
                this = (at + step >= 0) & (at + step < size)
                ok = this if ok is None else ok & this
        return ok

    def greet(semaphore, reach):
        for dy in (reach, -reach):
            @pl.when(there(0, dy))
            def _(dy=dy):
                pl.semaphore_signal(semaphore, inc=1, device_id=(gx, gy + dy), device_id_type=MESH)

    def greeted(semaphore, reach, more=0):
        present = (gy >= reach).astype(jnp.int32) + (gy + reach < ny).astype(jnp.int32)
        pl.semaphore_wait(semaphore, present + more)

    @pl.loop(0, nx, unroll=nx <= 16)
    def _(x):
        @pl.when(x != gx)
        def _():
            pl.semaphore_signal(barrier, inc=1, device_id=(x, gy), device_id_type=MESH)

    greet(barrier, 1)
    piece = bx // PIECES
    for c in ORDER:
        for src, main, end in ((b_ref, f0m, f0t), (d_ref, ddm, ddt)):
            for to, lanes in ((main, pl.ds(0, LANES)), (end, pl.ds(LANES, tail))):
                pltpu.make_async_copy(
                    src.at[pl.ds(c * piece, piece), :, lanes],
                    to.at[pl.ds(1 + c * piece, piece), pl.ds(ROWS, by), :], own_sem.at[c]).start()

    lane = lax.broadcasted_iota(jnp.int32, (CHUNK, LANES), 1)
    row = lax.broadcasted_iota(jnp.int32, (CHUNK, LANES), 0)

    def zeros(*shape):
        return jnp.zeros(shape, jnp.float32)

    def rolled(x, by_lanes):
        return pltpu.roll(x, by_lanes, axis=1)

    def widen(x):
        return jnp.concatenate([x, zeros(x.shape[0], LANES - tail)], 1)

    def cut(x):
        return jnp.where(lane[:x.shape[0]] < tail, x, 0.0)

    flat_f = (f0m.reshape(high * deep, LANES), f0t.reshape(high * deep, tail))
    flat_d = (ddm.reshape(high * deep, LANES), ddt.reshape(high * deep, tail))
    flat_1 = v1.reshape(2, high * deep, LANES)
    flat_2 = v2.reshape(2, high * deep, LANES)
    flat_3 = v3.reshape(2, bx * by, LANES)

    def along(at, k=0, size=None):
        return pl.ds((k + 1) * deep + at, size or bx, stride=deep)

    def strip_f(t, at):
        return widen(flat_f[1][along(at)]) if t else flat_f[0][along(at)]

    def strip_d(t, at, k=0, size=None):
        rows = along(at, k, size)
        return widen(flat_d[1][rows]) if t else flat_d[0][rows]

    for at in (first - 1, last + 1):
        flat_f[0][along(at)] = zeros(bx, LANES)
        flat_f[1][along(at)] = zeros(bx, tail)
        for t in two:
            flat_1[t, along(at)] = zeros(bx, LANES)
            flat_2[t, along(at)] = zeros(bx, LANES)
            ex[t, at:at + 1] = zeros(1, LANES)
    for side in two:
        @pl.when(jnp.logical_not(x_ok[side]))
        def _(side=side):
            xr[side] = zeros(*xr.shape[1:])
            fx[side] = zeros(*fx.shape[1:])

        @pl.when(jnp.logical_not(y_ok[side]))
        def _(side=side):
            yr[side] = zeros(*yr.shape[1:])
            fyr[side] = zeros(*fyr.shape[1:])
    for c, (dx, dy) in enumerate(CORNERS):
        @pl.when(x_ok[dx < 0] & jnp.logical_not(y_ok[dy < 0]))
        def _(c=c, dx=dx):
            xr[int(dx < 0), pl.ds(part_x * 2 + 8 * (c // 2), 8)] = zeros(8, LANES)

    def f0(t, layer, start, size):
        rows = pl.ds(start, size)
        return widen(f0t[layer, rows]) if t else f0m[layer, rows]

    def dd(t, layer, start, size):
        rows = pl.ds(start, size)
        return widen(ddt[layer, rows]) if t else ddm[layer, rows]

    def g1(t, layer, start, size):
        return v1[t, layer, pl.ds(start, size)]

    def g2(t, layer, start, size):
        return v2[t, layer, pl.ds(start, size)]

    def beside_z(a, b):
        at = lane[:a.shape[0]]
        left_a, left_b = rolled(a, 1), rolled(b, 1)
        right_a, right_b = rolled(a, LANES - 1), rolled(b, LANES - 1)
        return (jnp.where(at == 0, left_b, left_a) + jnp.where(at == LANES - 1, right_b, right_a),
                jnp.where(at == 0, left_a, left_b) + right_b)

    def times_b(shift, here, others):
        z = beside_z(*here)
        out = []
        for t in two:
            total = z[t]
            for o in others:
                total = total + o[t]
            out.append(shift[t] * here[t] - total)
        return out[0], cut(out[1])

    def apply(field, layer, start, size, steps):
        def get(layer, start):
            return [field(t, layer, start, size) for t in two]

        others = [get(layer, start - 1), get(layer, start + 1)] + [get(layer + step, start) for step in steps]
        return times_b([dd(t, layer, start, size) for t in two], get(layer, start), others)

    def within(k):
        return (1,) if k == 0 else (-1,) if k == bx - 1 else (-1, 1)

    def pack(buffer, at, main, end):
        size = main.shape[0]
        half = size // 2
        low, up = end[:half], rolled(end[half:], tail)
        buffer[at:at + size] = main
        buffer[at + size:at + size + half] = jnp.where(
            lax.broadcasted_iota(jnp.int32, (half, LANES), 1) < tail, low, up)

    def unpack(buffer, at, size):
        half = size // 2
        both = buffer[at + size:at + size + half]
        keep = lax.broadcasted_iota(jnp.int32, (half, LANES), 1) < tail
        end = [jnp.where(keep, e, 0.0) for e in (both, rolled(both, LANES - tail))]
        return buffer[at:at + size], jnp.concatenate(end, 0)

    def x_copies(d):
        return [pltpu.make_async_remote_copy(
            src_ref=xs.at[d, rows], dst_ref=xr.at[d, rows], send_sem=x_send.at[0], recv_sem=x_recv.at[d + 2 * n],
            device_id=(gx + 1 - 2 * d, gy), device_id_type=MESH)
            for n, rows in enumerate((pl.ds(0, by * 3), pl.ds(by * 3, x_half * 3)))]

    def y_copies(d):
        return [pltpu.make_async_remote_copy(
            src_ref=ys.at[d], dst_ref=yr.at[d], send_sem=y_send.at[0], recv_sem=y_recv.at[0],
            device_id=(gx, gy + 1 - 2 * d), device_id_type=MESH)]

    def start(make, at):
        @pl.when(at)
        def _():
            for copy in make():
                copy.start()

    def wait_all(ref, present, sizes, semaphore):
        for n in sizes:
            @pl.when(present == n)
            def _(n=n):
                some = ref.at[pl.ds(0, n)]
                pltpu.make_async_copy(some, some, semaphore.at[0]).wait()

    stages = relay_reaches(ny)
    entered = [0]

    def enter():
        n = entered[0]
        if 0 < n <= len(stages):
            greeted(ready.at[n - 1], stages[n - 1])
        if n < len(stages):
            greet(ready.at[n], stages[n])
        entered[0] += 1

    def come(c):
        some = b_ref.at[pl.ds(0, 2 * piece)]
        pltpu.make_async_copy(some, some, own_sem.at[c]).wait()

    here, done = set(), set()
    for n, c in enumerate(ORDER):
        come(c)
        here |= set(range(c * piece, (c + 1) * piece))
        for k in range(bx):
            if k in done or not {max(k - 1, 0), k, min(k + 1, bx - 1)} <= here:
                continue
            done.add(k)
            for at in range(first, first + by, CHUNK):
                out = apply(f0, k + 1, at, CHUNK, within(k))
                for t in two:
                    v1[t, k + 1, pl.ds(at, CHUNK)] = out[t]
        if n != 1:
            continue
        for d in two:
            _, edge, inner = x_side[1 - d]
            half = first + d * x_half
            for at, size, one, one_at, two_, two_at in (
                    (0, by, f0, first, edge, first), (by * 3, x_half, dd, half, inner, half)):
                for n in range(0, size, CHUNK):
                    a = [one(t, edge, one_at + n, CHUNK) for t in two]
                    b = [g1(t, two_, two_at + n, CHUNK) for t in two]
                    xs[d, pl.ds(at + n, CHUNK)] = a[0]
                    xs[d, pl.ds(at + size + n, CHUNK)] = b[0]
                    xs[d, pl.ds(at + 2 * size + n, CHUNK)] = jnp.where(lane < tail, a[1], rolled(b[1], tail))
        for c, (dx, dy) in enumerate(CORNERS):
            _, edge, inner = x_side[dx > 0]
            _, near, next_ = y_side[dy > 0]
            for n, (field, layer, at) in enumerate(
                    ((f0, edge, near), (g1, edge, near), (f0, inner, near), (f0, edge, next_))):
                for t in two:
                    cs[c, 4 * t + n:4 * t + n + 1] = field(t, layer, at, 1)
        greeted(barrier, 1, nx - 1)
        for d in two:
            start(functools.partial(x_copies, d), x_ok[1 - d])
        enter()
    for d in two:
        _, edge, inner = y_side[1 - d]
        pack(ys.at[d], 0, *(strip_f(t, edge) for t in two))
        pack(ys.at[d], bx * 3 // 2, *(strip_d(t, edge, d * y_half, y_half) for t in two))
        pack(ys.at[d], part_y, *(flat_1[t, along(edge)] for t in two))
        pack(ys.at[d], part_y + bx * 3 // 2, *(flat_1[t, along(inner, d * y_half, y_half)] for t in two))
        start(functools.partial(y_copies, d), y_ok[1 - d])

    sums = [zeros(8, LANES)] * 6

    def add(n, a, b):
        total = sums[n]
        for t in two:
            product = a[t] * b[t]
            for g in range(product.shape[0] // 8):
                total = total + product[8 * g:8 * g + 8]
        sums[n] = total

    def moments(k, which, begin, end, size=CHUNK):
        layer = k + 1
        for at in range(first + begin, first + end, size):
            fields = {}

            def get(n):
                if n not in fields:
                    fields[n] = [(f0, g1, g2)[n](t, layer, at, size) for t in two]
                return fields[n]

            for n in which:
                if n < 5:
                    add(n, get(n // 2), get((n + 1) // 2))
                else:
                    a, b = get(2)
                    left_a, left_b = rolled(a, 1), rolled(b, 1)
                    edge = lane[:size] == 0
                    z = (jnp.where(edge, left_b, left_a), jnp.where(edge, left_a, left_b))
                    value = []
                    for t in two:
                        other = z[t] + g2(t, layer, at - 1, size)
                        if k > 2:
                            other = other + g2(t, layer - 1, at, size)
                        value.append(dd(t, layer, at, size) * get(2)[t] - (other + other))
                    add(5, get(2), value)

    enter()
    for c, (dx, dy) in enumerate(CORNERS):
        start(lambda: [pltpu.make_async_remote_copy(
            src_ref=cs.at[c], dst_ref=xr.at[int(dx < 0), pl.ds(part_x * 2 + 8 * (c // 2), 8)],
            send_sem=c_send.at[0], recv_sem=x_recv.at[int(dx < 0)],
            device_id=(gx + dx, gy + dy), device_id_type=MESH)], there(dx, dy))
    for k in range(bx):
        for at in range(first, first + by, CHUNK):
            out = apply(g1, k + 1, at, CHUNK, within(k))
            for t in two:
                v2[t, k + 1, pl.ds(at, CHUNK)] = out[t]
        moments(k, (0,), 0, by)
    def which(k):
        return (1, 2) + ((3, 4, 5) if 1 < k < bx - 2 else ())

    for k in range(1, bx - 1):
        moments(k, which(k), 8, by - 8)

    def corner(side, other, n):
        return [xr[side, pl.ds(part_x * 2 + 8 * other + 4 * t + n, 1)] for t in two]

    wait_all(yr, y_count, (1, 2), y_recv)
    for side in two:
        _, edge, inner = y_side[side]
        e, g = unpack(yr.at[side], 0, bx), unpack(yr.at[side], part_y, bx)
        field = [strip_f(t, edge) for t in two]
        f1h = [jnp.where(y_ok[side], g[t] - field[t], 0.0) for t in two]
        shift = lambda x: [jnp.concatenate([zeros(1, LANES), x[:-1]], 0), jnp.concatenate([x[1:], zeros(1, LANES)], 0)]
        moved = [shift(x) for x in e]
        spread = times_b([strip_d(t, edge) for t in two], e, [[m[n] for m in moved] for n in two])
        for t in two:
            flat_1[t, along(edge)] = flat_1[t, along(edge)] - e[t]
            flat_2[t, along(edge)] = flat_2[t, along(edge)] - spread[t] - f1h[t]
            flat_2[t, along(inner)] = flat_2[t, along(inner)] + e[t]
            ey[side, t] = e[t]
            hy[side, t, 1:bx + 1] = f1h[t]
    for begin in (0, by - 8):
        for k in range(1, bx - 1):
            moments(k, which(k), begin, begin + 8, 8)

    def x_phase(turn, carry):
        sums[:] = carry
        odd = lax.rem(gx, 2)
        side = jnp.where(turn == 0, 1 - odd, odd)
        upper = side == 1

        def either(low, up):
            return jnp.where(upper, up, low)

        ok = either(gx, nx - 1 - gx) > 0
        halo, edge, inner, third = (either(n, bx + 1 - n) for n in range(4))
        beyond, near = either(first - 1, last + 1), either(first, last)
        ok_y = either(gy, ny - 1 - gy) > 0

        @pl.when(ok)
        def _():
            for n in (0, 1, 2):
                @pl.when(y_count == n)
                def _(n=n):
                    some = xr.at[0, pl.ds(0, by * 3 + 8 * n)]
                    pltpu.make_async_copy(some, some, x_recv.at[side]).wait()

        def got(at, size, n):
            end = xr[side, pl.ds(at + 2 * size + n, CHUNK)]
            return ((xr[side, pl.ds(at + n, CHUNK)], cut(end)),
                    (xr[side, pl.ds(at + size + n, CHUNK)], cut(rolled(end, LANES - tail))))

        chunks = [got(0, by, at) for at in range(0, by, CHUNK)]
        for n, (e, _) in enumerate(chunks):
            for t in two:
                ex[t, pl.ds(first + n * CHUNK, CHUNK)] = e[t]
        for at, (here, g) in zip(range(0, by, CHUNK), chunks):
            rows = pl.ds(first + at, CHUNK)
            others = [[ex[t, pl.ds(first + at + step, CHUNK)] for t in two] for step in (-1, 1)]
            spread = times_b([dd(t, edge, first + at, CHUNK) for t in two], here, others)
            for t in two:
                f1h = jnp.where(ok, g[t] - f0(t, edge, first + at, CHUNK), 0.0)
                v1[t, halo, rows] = f1h
                v1[t, edge, rows] = v1[t, edge, rows] - here[t]
                v2[t, edge, rows] = v2[t, edge, rows] - spread[t] - f1h
                v2[t, inner, rows] = v2[t, inner, rows] + here[t]
        for other, at in ((0, near), (1, first + last - near)):
            for t in two:
                p = corner(side, other, 0)[t]
                v1[t, halo, pl.ds(at, 1)] = v1[t, halo, pl.ds(at, 1)] - p
                v2[t, edge, pl.ds(at, 1)] = v2[t, edge, pl.ds(at, 1)] + (p + p)
        for t in two:
            value = corner(side, 0, 1)[t] - ey[side, t, pl.ds(edge - 1, 1)] - ex[t, pl.ds(near, 1)]
            value = jnp.where(ok & ok_y, value, 0.0)
            v1[t, halo, pl.ds(beyond, 1)] = value
            hy[side, t, pl.ds(halo, 1)] = value
            hy[side, t, pl.ds(edge, 1)] = hy[side, t, pl.ds(edge, 1)] - corner(side, 0, 0)[t]
        k = side * y_half
        shift = unpack(yr.at[side], bx * 3 // 2, y_half)
        far = unpack(yr.at[side], part_y + bx * 3 // 2, y_half)
        here, *moved = [[hy[side, t, pl.ds(k + step, y_half)] for t in two] for step in (1, 0, 2)]
        inside = [flat_1[t, along(near, k, y_half)] for t in two]
        out = times_b(shift, here, moved + [inside, far])
        value = []
        for t in two:
            o = out[t] + jnp.where(row[:y_half] + k == edge - 1, corner(side, 0, 3)[t], 0.0)
            o = jnp.where(ok_y, o, 0.0)
            fy[side, t] = o
            value.append(o)
        add(5, [-2.0 * flat_2[t, along(near, k, y_half)] for t in two], value)

        for at in range(first, first + by, CHUNK):
            zero, one, two_e, two_i = (
                [field(t, layer, at, CHUNK) for t in two]
                for field, layer in ((f0, edge), (g1, edge), (g2, edge), (g2, inner)))
            one_i, two_t = ([field(t, layer, at, CHUNK) for t in two] for field, layer in ((g1, inner), (g2, third)))
            add(1, zero, one)
            add(2, one, one)
            for layer, f1_, f2_, next_ in ((edge, one, two_e, two_i), (inner, one_i, two_i, two_t)):
                add(3, f1_, f2_)
                add(4, f2_, f2_)
                left_a, left_b = rolled(f2_[0], 1), rolled(f2_[1], 1)
                z = (jnp.where(lane == 0, left_b, left_a), jnp.where(lane == 0, left_a, left_b))
                value = []
                for t in two:
                    other = z[t] + g2(t, layer, at - 1, CHUNK) + next_[t]
                    value.append(dd(t, layer, at, CHUNK) * f2_[t] - (other + other))
                add(5, f2_, value)

        parts = []
        more = corner(side, 0, 2)
        for at in range(0, x_half, CHUNK):
            begin = first + side * x_half + at
            f1h = [g1(t, halo, begin, CHUNK) for t in two]
            z = beside_z(*f1h)
            so_far = []
            for t in two:
                near_by = z[t] + g1(t, halo, begin - 1, CHUNK) + g1(t, halo, begin + 1, CHUNK)
                near_by = near_by + g1(t, edge, begin, CHUNK)
                so_far.append(near_by - jnp.where(row + begin == near, more[t], 0.0))
            parts.append((begin, f1h, so_far, [-2.0 * g2(t, edge, begin, CHUNK) for t in two]))

        @pl.when(ok)
        def _():
            some = xr.at[0, pl.ds(0, x_half * 3)]
            pltpu.make_async_copy(some, some, x_recv.at[2 + side]).wait()

        for n, (begin, f1h, so_far, weight) in enumerate(parts):
            shift, far = got(by * 3, x_half, n * CHUNK)
            value = [shift[t] * f1h[t] - so_far[t] - far[t] for t in two]
            value = [jnp.where(ok, v, 0.0) for v in (value[0], cut(value[1]))]
            for t in two:
                fx[side, t, pl.ds(begin - first, CHUNK)] = value[t]
            add(5, weight, value)
        return tuple(sums)

    sums[:] = lax.fori_loop(0, 2, x_phase, tuple(sums))

    while entered[0] <= len(stages):
        enter()
    lane_of = lane[:8]
    row_of = row[:8]
    stacked = zeros(8, LANES)
    for n, s in enumerate(sums):
        stacked = jnp.where(row_of == n, jnp.sum(s, 0, keepdims=True), stacked)
    packed = jnp.sum(jnp.where(lane_of == row_of, jnp.sum(stacked, 1, keepdims=True), 0.0), 0, keepdims=True)
    part[...] = packed

    @pl.loop(0, nx, unroll=nx * ny <= 64)
    def _(x):
        @pl.loop(0, ny, unroll=nx * ny <= 64)
        def _(y):
            @pl.when((x != gx) | (y != gy))
            def _():
                pltpu.make_async_remote_copy(
                    src_ref=part, dst_ref=slots.at[pl.ds(me, 1)], send_sem=sum_send.at[0],
                    recv_sem=sum_recv.at[0], device_id=(x, y), device_id_type=MESH).start()

    slots[pl.ds(me, 1)] = packed
    for d in two:
        _, edge, _ = x_side[1 - d]
        rows = pl.ds((1 - d) * x_half, x_half)
        start(lambda: [pltpu.make_async_remote_copy(
            src_ref=v2.at[:, edge, pl.ds(first + (1 - d) * x_half, x_half)], dst_ref=fx.at[d, :, rows],
            send_sem=fx_send.at[0], recv_sem=fx_recv.at[0],
            device_id=(gx + 1 - 2 * d, gy), device_id_type=MESH)], x_ok[1 - d])
        _, edge, _ = y_side[1 - d]
        for t in two:
            fys[d, t] = flat_2[t, along(edge, (1 - d) * y_half, y_half)]
        start(lambda: [pltpu.make_async_remote_copy(
            src_ref=fys.at[d], dst_ref=fyr.at[d], send_sem=fy_send.at[0], recv_sem=fy_recv.at[0],
            device_id=(gx, gy + 1 - 2 * d), device_id_type=MESH)], y_ok[1 - d])

    for k in range(bx):
        for at in range(first, first + by, CHUNK):
            out = apply(g2, k + 1, at, CHUNK, within(k))
            for t in two:
                v3[t, k, pl.ds(at - first, CHUNK)] = out[t]

    wait_all(xs, x_count, (1, 2), x_send)
    wait_all(ys, y_count, (1, 2), y_send)
    wait_all(cs, x_count * y_count, (1, 2, 4), c_send)
    half_x, half_y = fx.at[:, :, pl.ds(0, x_half)], fys
    wait_all(half_x, x_count, (1, 2), fx_send)
    wait_all(half_y, y_count, (1, 2), fy_send)
    others = slots.at[pl.ds(0, count - 1)]
    pltpu.make_async_copy(others, others, sum_send.at[0]).wait()
    wait_all(half_x, x_count, (1, 2), fx_recv)
    wait_all(half_y, y_count, (1, 2), fy_recv)
    for side in two:
        edge = x_side[side][1] - 1
        for t in two:
            v3[t, edge] = v3[t, edge] - fx[side, t]
        edge = y_side[side][1] - first
        for t in two:
            pieces = [fy[side, t], fyr[side, t]]
            rows = pl.ds(edge, bx, stride=by)
            flat_3[t, rows] = flat_3[t, rows] - jnp.concatenate(pieces[::-1] if side else pieces, 0)

    pltpu.make_async_copy(others, others, sum_recv.at[0]).wait()
    total = jnp.sum(slots[...], 0, keepdims=True)
    moment = [jnp.broadcast_to(total[:, k:k + 1], (1, LANES)) for k in range(6)]
    co = zeros(8, LANES)
    for k, c in enumerate(coefficients(moment)):
        co = jnp.where(row_of == k, c, co)
    co_ref[...] = co


def combine(f0m, f0t, v1, v2, v3, co_ref, x_out, r_out, x_buf, r_buf, sems):
    bx, by, bz = x_out.shape
    tail = bz - LANES
    c = [jnp.broadcast_to(co_ref[k:k + 1, :], (by, LANES)) for k in range(7)]
    rows = pl.ds(ROWS, by)

    def copy(n, k):
        src, dst = ((x_buf, x_out), (r_buf, r_out))[n]
        return pltpu.make_async_copy(src.at[pl.ds(k, 1)], dst.at[pl.ds(k, 1)], sems.at[n])

    for k in range(bx):
        for t in range(2):
            wide = LANES if t == 0 else tail
            lanes = slice(LANES * t, LANES * t + wide)
            f0 = f0t[k + 1, rows] if t else f0m[k + 1, rows]
            f1, f2, f3 = (v1[t, k + 1, rows], v2[t, k + 1, rows], v3[t, k])
            m = [a[:, :wide] for a in c]
            f1, f2, f3 = f1[:, :wide], f2[:, :wide], f3[:, :wide]
            x_buf[k, :, lanes] = m[0] * f0 + m[1] * f1 + m[2] * f2
            r_buf[k, :, lanes] = m[3] * f0 + m[4] * f1 + m[5] * f2 + m[6] * f3
        for n in range(2):
            copy(n, k).start()
    for n, (src, dst) in enumerate(((x_buf, x_out), (r_buf, r_out))):
        pltpu.make_async_copy(src, dst, sems.at[n]).wait()


def on_device(nx, ny, right_side, diagonal):
    bx, by, bz = right_side.shape
    tail = bz - LANES
    f32 = jnp.float32
    block = jax.ShapeDtypeStruct((bx, by, bz), f32)
    high, deep = bx + 2, by + 3 * ROWS
    vmem = pl.BlockSpec(memory_space=pltpu.VMEM)
    dma = pltpu.SemaphoreType.DMA
    shape = lambda *dims: jax.ShapeDtypeStruct(dims, f32)
    space = lambda *dims: pltpu.VMEM(dims, f32)
    x_rows, y_rows = by * 9 // 2, bx * 9 // 2
    fields = pl.pallas_call(
        functools.partial(kernel, nx, ny),
        out_shape=(shape(high, deep, LANES), shape(high, deep, tail), shape(2, high, deep, LANES),
                   shape(2, high, deep, LANES), shape(2, bx, by, LANES), shape(8, LANES)),
        in_specs=[pl.BlockSpec(memory_space=pltpu.HBM)] * 2,
        out_specs=(vmem,) * 6,
        scratch_shapes=[
            space(high, deep, LANES), space(high, deep, tail),
            space(2, x_rows, LANES), space(2, x_rows + 16, LANES), space(2, y_rows, LANES), space(2, y_rows, LANES),
            space(4, 8, LANES),
            space(2, deep, LANES), space(2, 2, bx, LANES), space(2, 2, bx + 2, LANES),
            space(2, 2, by, LANES), space(2, 2, bx // 2, LANES),
            space(2, 2, bx // 2, LANES), space(2, 2, bx // 2, LANES),
            space(1, LANES), space(nx * ny, LANES),
            dma((PIECES,)), dma((1,)), dma((4,)), dma((1,)), dma((1,)), dma((1,)), *[dma((1,))] * 6,
            pltpu.SemaphoreType.REGULAR((len(relay_reaches(ny)),)),
        ],
        compiler_params=pltpu.CompilerParams(
            collective_id=0, has_side_effects=True, vmem_limit_bytes=32 * 2**20),
    )(*(pltpu.with_memory_space_constraint(a, pltpu.HBM) for a in (right_side, diagonal)))
    return pl.pallas_call(
        combine,
        out_shape=(block, block),
        in_specs=[vmem] * 6,
        out_specs=(pl.BlockSpec(memory_space=pl.ANY),) * 2,
        scratch_shapes=[space(bx, by, bz), space(bx, by, bz), dma((2,))],
        compiler_params=pltpu.CompilerParams(vmem_limit_bytes=24 * 2**20),
    )(*fields)


def solution(mesh):
    placed = (P("gx", "gy", None), P("gx", "gy", None))
    return jax.shard_map(
        functools.partial(on_device, mesh.shape["gx"], mesh.shape["gy"]),
        mesh=mesh,
        in_specs=placed,
        out_specs=placed,
        check_vma=False,
    )
```

```python
import functools

import jax
import jax.numpy as jnp
from jax import lax
from jax.experimental import pallas as pl
from jax.experimental.pallas import tpu as pltpu
from jax.sharding import PartitionSpec as P

SHIFT = 6.0
MESH = pl.DeviceIdType.MESH
DIRS = ((1, 0), (-1, 0), (0, 1), (0, -1), (1, 1), (1, -1), (-1, 1), (-1, -1))
CORNERS = ((1, 1), (-1, -1), (1, -1), (-1, 1))
ROWS = 8
LANES = 128
CHUNK = 16
PIECES = 4
ORDER = (3, 0, 1, 2)


def relay_reaches(ny):
    return [2 ** n for n in range((ny - 1).bit_length())]


def coefficients(m):
    a = [m[k + 1] + SHIFT * m[k] for k in range(5)]
    inverse0 = 1.0 / a[0]
    lower1, lower2 = a[1] * inverse0, a[2] * inverse0
    inverse1 = 1.0 / (a[2] - a[1] * lower1)
    across = a[3] - a[2] * lower1
    right1, right2 = m[1] - m[0] * lower1, m[2] - m[0] * lower2
    lower3 = across * inverse1
    x2 = (right2 - right1 * lower3) / (a[4] - a[2] * lower2 - across * lower3)
    x1 = (right1 - across * x2) * inverse1
    x0 = (m[0] - a[1] * x1 - a[2] * x2) * inverse0
    return x0, x1, x2, 1.0 - SHIFT * x0, -SHIFT * x1 - x0, -SHIFT * x2 - x1, -x2


def kernel(nx, ny, b_ref, d_ref, f0m, f0t, v1, v2, v3, co_ref,
           ddm, ddt, xs, xr, ys, yr, cs, ex, ey, hy, fx, fy, fys, fyr, part, slots,
           own_sem, x_send, x_recv, y_send, y_recv, c_send,
           fx_send, fx_recv, fy_send, fy_recv, sum_send, sum_recv, ready):
    gx, gy = lax.axis_index("gx"), lax.axis_index("gy")
    bx, by, bz = b_ref.shape
    tail = bz - LANES
    high, deep = f0m.shape[:2]
    two = range(2)
    barrier = pltpu.get_barrier_semaphore()
    count = nx * ny
    me = gx * ny + gy
    x_ok, y_ok = (gx > 0, gx < nx - 1), (gy > 0, gy < ny - 1)
    x_count, y_count = (sum(o.astype(jnp.int32) for o in ok) for ok in (x_ok, y_ok))
    first, last = ROWS, ROWS + by - 1
    x_side = ((0, 1, 2), (bx + 1, bx, bx - 1))
    y_side = ((first - 1, first, first + 1), (last + 1, last, last - 1))
    x_half, y_half = by // 2, bx // 2
    part_x, part_y = by * 9 // 4, bx * 9 // 4

    def there(dx, dy):
        ok = None
        for at, step, size in ((gx, dx, nx), (gy, dy, ny)):
            if step:
                this = (at + step >= 0) & (at + step < size)
                ok = this if ok is None else ok & this
        return ok

    def greet(semaphore, reach):
        for dy in (reach, -reach):
            @pl.when(there(0, dy))
            def _(dy=dy):
                pl.semaphore_signal(semaphore, inc=1, device_id=(gx, gy + dy), device_id_type=MESH)

    def greeted(semaphore, reach, more=0):
        present = (gy >= reach).astype(jnp.int32) + (gy + reach < ny).astype(jnp.int32)
        pl.semaphore_wait(semaphore, present + more)

    @pl.loop(0, nx, unroll=nx <= 16)
    def _(x):
        @pl.when(x != gx)
        def _():
            pl.semaphore_signal(barrier, inc=1, device_id=(x, gy), device_id_type=MESH)

    greet(barrier, 1)
    piece = bx // PIECES
    for c in ORDER:
        for src, main, end in ((b_ref, f0m, f0t), (d_ref, ddm, ddt)):
            for to, lanes in ((main, pl.ds(0, LANES)), (end, pl.ds(LANES, tail))):
                pltpu.make_async_copy(
                    src.at[pl.ds(c * piece, piece), :, lanes],
                    to.at[pl.ds(1 + c * piece, piece), pl.ds(ROWS, by), :], own_sem.at[c]).start()

    lane = lax.broadcasted_iota(jnp.int32, (CHUNK, LANES), 1)
    row = lax.broadcasted_iota(jnp.int32, (CHUNK, LANES), 0)

    def zeros(*shape):
        return jnp.zeros(shape, jnp.float32)

    def rolled(x, by_lanes):
        return pltpu.roll(x, by_lanes, axis=1)

    def widen(x):
        return jnp.concatenate([x, zeros(x.shape[0], LANES - tail)], 1)

    def cut(x):
        return jnp.where(lane[:x.shape[0]] < tail, x, 0.0)

    flat_f = (f0m.reshape(high * deep, LANES), f0t.reshape(high * deep, tail))
    flat_d = (ddm.reshape(high * deep, LANES), ddt.reshape(high * deep, tail))
    flat_1 = v1.reshape(2, high * deep, LANES)
    flat_2 = v2.reshape(2, high * deep, LANES)
    flat_3 = v3.reshape(2, bx * by, LANES)

    def along(at, k=0, size=None):
        return pl.ds((k + 1) * deep + at, size or bx, stride=deep)

    def strip_f(t, at):
        return widen(flat_f[1][along(at)]) if t else flat_f[0][along(at)]

    def strip_d(t, at, k=0, size=None):
        rows = along(at, k, size)
        return widen(flat_d[1][rows]) if t else flat_d[0][rows]

    for at in (first - 1, last + 1):
        flat_f[0][along(at)] = zeros(bx, LANES)
        flat_f[1][along(at)] = zeros(bx, tail)
        for t in two:
            flat_1[t, along(at)] = zeros(bx, LANES)
            flat_2[t, along(at)] = zeros(bx, LANES)
            ex[t, at:at + 1] = zeros(1, LANES)
    for side in two:
        @pl.when(jnp.logical_not(x_ok[side]))
        def _(side=side):
            xr[side] = zeros(*xr.shape[1:])
            fx[side] = zeros(*fx.shape[1:])

        @pl.when(jnp.logical_not(y_ok[side]))
        def _(side=side):
            yr[side] = zeros(*yr.shape[1:])
            fyr[side] = zeros(*fyr.shape[1:])
    for c, (dx, dy) in enumerate(CORNERS):
        @pl.when(x_ok[dx < 0] & jnp.logical_not(y_ok[dy < 0]))
        def _(c=c, dx=dx):
            xr[int(dx < 0), pl.ds(part_x * 2 + 8 * (c // 2), 8)] = zeros(8, LANES)

    def f0(t, layer, start, size):
        rows = pl.ds(start, size)
        return widen(f0t[layer, rows]) if t else f0m[layer, rows]

    def dd(t, layer, start, size):
        rows = pl.ds(start, size)
        return widen(ddt[layer, rows]) if t else ddm[layer, rows]

    def g1(t, layer, start, size):
        return v1[t, layer, pl.ds(start, size)]

    def g2(t, layer, start, size):
        return v2[t, layer, pl.ds(start, size)]

    def beside_z(a, b):
        at = lane[:a.shape[0]]
        left_a, left_b = rolled(a, 1), rolled(b, 1)
        right_a, right_b = rolled(a, LANES - 1), rolled(b, LANES - 1)
        return (jnp.where(at == 0, left_b, left_a) + jnp.where(at == LANES - 1, right_b, right_a),
                jnp.where(at == 0, left_a, left_b) + right_b)

    def times_b(shift, here, others):
        z = beside_z(*here)
        out = []
        for t in two:
            total = z[t]
            for o in others:
                total = total + o[t]
            out.append(shift[t] * here[t] - total)
        return out[0], cut(out[1])

    def apply(field, layer, start, size, steps):
        def get(layer, start):
            return [field(t, layer, start, size) for t in two]

        others = [get(layer, start - 1), get(layer, start + 1)] + [get(layer + step, start) for step in steps]
        return times_b([dd(t, layer, start, size) for t in two], get(layer, start), others)

    def within(k):
        return (1,) if k == 0 else (-1,) if k == bx - 1 else (-1, 1)

    def pack(buffer, at, main, end):
        size = main.shape[0]
        half = size // 2
        low, up = end[:half], rolled(end[half:], tail)
        buffer[at:at + size] = main
        buffer[at + size:at + size + half] = jnp.where(
            lax.broadcasted_iota(jnp.int32, (half, LANES), 1) < tail, low, up)

    def unpack(buffer, at, size):
        half = size // 2
        both = buffer[at + size:at + size + half]
        keep = lax.broadcasted_iota(jnp.int32, (half, LANES), 1) < tail
        end = [jnp.where(keep, e, 0.0) for e in (both, rolled(both, LANES - tail))]
        return buffer[at:at + size], jnp.concatenate(end, 0)

    late = lax.rem(gx, 8) == 2

    def x_copies(d):
        return [pltpu.make_async_remote_copy(
            src_ref=xs.at[d, rows], dst_ref=xr.at[d, rows], send_sem=x_send.at[0], recv_sem=x_recv.at[d + 2 * n],
            device_id=(gx + 1 - 2 * d, gy), device_id_type=MESH)
            for n, rows in enumerate((pl.ds(0, by * 3), pl.ds(by * 3, x_half * 3)))]

    def y_copies(d):
        return [pltpu.make_async_remote_copy(
            src_ref=ys.at[d], dst_ref=yr.at[d], send_sem=y_send.at[0], recv_sem=y_recv.at[0],
            device_id=(gx, gy + 1 - 2 * d), device_id_type=MESH)]

    def start(make, at):
        @pl.when(at)
        def _():
            for copy in make():
                copy.start()

    def wait_all(ref, present, sizes, semaphore):
        for n in sizes:
            @pl.when(present == n)
            def _(n=n):
                some = ref.at[pl.ds(0, n)]
                pltpu.make_async_copy(some, some, semaphore.at[0]).wait()

    stages = relay_reaches(ny)
    entered = [0]

    def enter():
        n = entered[0]
        if 0 < n <= len(stages):
            greeted(ready.at[n - 1], stages[n - 1])
        if n < len(stages):
            greet(ready.at[n], stages[n])
        entered[0] += 1

    def come(c):
        some = b_ref.at[pl.ds(0, 2 * piece)]
        pltpu.make_async_copy(some, some, own_sem.at[c]).wait()

    here, done = set(), set()
    for n, c in enumerate(ORDER):
        come(c)
        here |= set(range(c * piece, (c + 1) * piece))
        for k in range(bx):
            if k in done or not {max(k - 1, 0), k, min(k + 1, bx - 1)} <= here:
                continue
            done.add(k)
            for at in range(first, first + by, CHUNK):
                out = apply(f0, k + 1, at, CHUNK, within(k))
                for t in two:
                    v1[t, k + 1, pl.ds(at, CHUNK)] = out[t]
        if n != 1:
            continue
        for d in two:
            _, edge, inner = x_side[1 - d]
            half = first + d * x_half
            for at, size, one, one_at, two_, two_at in (
                    (0, by, f0, first, edge, first), (by * 3, x_half, dd, half, inner, half)):
                for n in range(0, size, CHUNK):
                    a = [one(t, edge, one_at + n, CHUNK) for t in two]
                    b = [g1(t, two_, two_at + n, CHUNK) for t in two]
                    xs[d, pl.ds(at + n, CHUNK)] = a[0]
                    xs[d, pl.ds(at + size + n, CHUNK)] = b[0]
                    xs[d, pl.ds(at + 2 * size + n, CHUNK)] = jnp.where(lane < tail, a[1], rolled(b[1], tail))
        for c, (dx, dy) in enumerate(CORNERS):
            _, edge, inner = x_side[dx > 0]
            _, near, next_ = y_side[dy > 0]
            for n, (field, layer, at) in enumerate(
                    ((f0, edge, near), (g1, edge, near), (f0, inner, near), (f0, edge, next_))):
                for t in two:
                    cs[c, 4 * t + n:4 * t + n + 1] = field(t, layer, at, 1)
        greeted(barrier, 1, nx - 1)
        start(functools.partial(x_copies, 0), x_ok[1])
        start(functools.partial(x_copies, 1), x_ok[0] & jnp.logical_not(late))
        enter()
    for d in two:
        _, edge, inner = y_side[1 - d]
        pack(ys.at[d], 0, *(strip_f(t, edge) for t in two))
        pack(ys.at[d], bx * 3 // 2, *(strip_d(t, edge, d * y_half, y_half) for t in two))
        pack(ys.at[d], part_y, *(flat_1[t, along(edge)] for t in two))
        pack(ys.at[d], part_y + bx * 3 // 2, *(flat_1[t, along(inner, d * y_half, y_half)] for t in two))
        start(functools.partial(y_copies, d), y_ok[1 - d])
    start(functools.partial(x_copies, 1), late)

    sums = [zeros(8, LANES)] * 6

    def add(n, a, b):
        total = sums[n]
        for t in two:
            product = a[t] * b[t]
            for g in range(product.shape[0] // 8):
                total = total + product[8 * g:8 * g + 8]
        sums[n] = total

    def moments(k, which, begin, end, size=CHUNK):
        layer = k + 1
        for at in range(first + begin, first + end, size):
            fields = {}

            def get(n):
                if n not in fields:
                    fields[n] = [(f0, g1, g2)[n](t, layer, at, size) for t in two]
                return fields[n]

            for n in which:
                if n < 5:
                    add(n, get(n // 2), get((n + 1) // 2))
                else:
                    a, b = get(2)
                    left_a, left_b = rolled(a, 1), rolled(b, 1)
                    edge = lane[:size] == 0
                    z = (jnp.where(edge, left_b, left_a), jnp.where(edge, left_a, left_b))
                    value = []
                    for t in two:
                        other = z[t] + g2(t, layer, at - 1, size)
                        if k > 2:
                            other = other + g2(t, layer - 1, at, size)
                        value.append(dd(t, layer, at, size) * get(2)[t] - (other + other))
                    add(5, get(2), value)

    enter()
    for c, (dx, dy) in enumerate(CORNERS):
        start(lambda: [pltpu.make_async_remote_copy(
            src_ref=cs.at[c], dst_ref=xr.at[int(dx < 0), pl.ds(part_x * 2 + 8 * (c // 2), 8)],
            send_sem=c_send.at[0], recv_sem=x_recv.at[int(dx < 0)],
            device_id=(gx + dx, gy + dy), device_id_type=MESH)], there(dx, dy))
    for k in range(bx):
        for at in range(first, first + by, CHUNK):
            out = apply(g1, k + 1, at, CHUNK, within(k))
            for t in two:
                v2[t, k + 1, pl.ds(at, CHUNK)] = out[t]
        moments(k, (0,), 0, by)
    def which(k):
        return (1, 2) + ((3, 4, 5) if 1 < k < bx - 2 else ())

    for k in range(1, bx - 1):
        moments(k, which(k), 8, by - 8)

    def corner(side, other, n):
        return [xr[side, pl.ds(part_x * 2 + 8 * other + 4 * t + n, 1)] for t in two]

    wait_all(yr, y_count, (1, 2), y_recv)
    for side in two:
        _, edge, inner = y_side[side]
        e, g = unpack(yr.at[side], 0, bx), unpack(yr.at[side], part_y, bx)
        field = [strip_f(t, edge) for t in two]
        f1h = [jnp.where(y_ok[side], g[t] - field[t], 0.0) for t in two]
        shift = lambda x: [jnp.concatenate([zeros(1, LANES), x[:-1]], 0), jnp.concatenate([x[1:], zeros(1, LANES)], 0)]
        moved = [shift(x) for x in e]
        spread = times_b([strip_d(t, edge) for t in two], e, [[m[n] for m in moved] for n in two])
        for t in two:
            flat_1[t, along(edge)] = flat_1[t, along(edge)] - e[t]
            flat_2[t, along(edge)] = flat_2[t, along(edge)] - spread[t] - f1h[t]
            flat_2[t, along(inner)] = flat_2[t, along(inner)] + e[t]
            ey[side, t] = e[t]
            hy[side, t, 1:bx + 1] = f1h[t]
    for begin in (0, by - 8):
        for k in range(1, bx - 1):
            moments(k, which(k), begin, begin + 8, 8)

    def x_phase(turn, carry):
        sums[:] = carry
        odd = lax.rem(gx, 2)
        lone = (gx == 0) | (gx == nx - 1)
        start_at = jnp.where(lone, odd, 1 - odd)
        side = jnp.where(turn == 0, start_at, 1 - start_at)
        upper = side == 1

        def either(low, up):
            return jnp.where(upper, up, low)

        ok = either(gx, nx - 1 - gx) > 0
        halo, edge, inner, third = (either(n, bx + 1 - n) for n in range(4))
        beyond, near = either(first - 1, last + 1), either(first, last)
        ok_y = either(gy, ny - 1 - gy) > 0

        @pl.when(ok)
        def _():
            for n in (0, 1, 2):
                @pl.when(y_count == n)
                def _(n=n):
                    some = xr.at[0, pl.ds(0, by * 3 + 8 * n)]
                    pltpu.make_async_copy(some, some, x_recv.at[side]).wait()

        def got(at, size, n):
            end = xr[side, pl.ds(at + 2 * size + n, CHUNK)]
            return ((xr[side, pl.ds(at + n, CHUNK)], cut(end)),
                    (xr[side, pl.ds(at + size + n, CHUNK)], cut(rolled(end, LANES - tail))))

        chunks = [got(0, by, at) for at in range(0, by, CHUNK)]
        for n, (e, _) in enumerate(chunks):
            for t in two:
                ex[t, pl.ds(first + n * CHUNK, CHUNK)] = e[t]
        for at, (here, g) in zip(range(0, by, CHUNK), chunks):
            rows = pl.ds(first + at, CHUNK)
            others = [[ex[t, pl.ds(first + at + step, CHUNK)] for t in two] for step in (-1, 1)]
            spread = times_b([dd(t, edge, first + at, CHUNK) for t in two], here, others)
            for t in two:
                f1h = jnp.where(ok, g[t] - f0(t, edge, first + at, CHUNK), 0.0)
                v1[t, halo, rows] = f1h
                v1[t, edge, rows] = v1[t, edge, rows] - here[t]
                v2[t, edge, rows] = v2[t, edge, rows] - spread[t] - f1h
                v2[t, inner, rows] = v2[t, inner, rows] + here[t]
        for other, at in ((0, near), (1, first + last - near)):
            for t in two:
                p = corner(side, other, 0)[t]
                v1[t, halo, pl.ds(at, 1)] = v1[t, halo, pl.ds(at, 1)] - p
                v2[t, edge, pl.ds(at, 1)] = v2[t, edge, pl.ds(at, 1)] + (p + p)
        for t in two:
            value = corner(side, 0, 1)[t] - ey[side, t, pl.ds(edge - 1, 1)] - ex[t, pl.ds(near, 1)]
            value = jnp.where(ok & ok_y, value, 0.0)
            v1[t, halo, pl.ds(beyond, 1)] = value
            hy[side, t, pl.ds(halo, 1)] = value
            hy[side, t, pl.ds(edge, 1)] = hy[side, t, pl.ds(edge, 1)] - corner(side, 0, 0)[t]
        k = side * y_half
        shift = unpack(yr.at[side], bx * 3 // 2, y_half)
        far = unpack(yr.at[side], part_y + bx * 3 // 2, y_half)
        here, *moved = [[hy[side, t, pl.ds(k + step, y_half)] for t in two] for step in (1, 0, 2)]
        inside = [flat_1[t, along(near, k, y_half)] for t in two]
        out = times_b(shift, here, moved + [inside, far])
        value = []
        for t in two:
            o = out[t] + jnp.where(row[:y_half] + k == edge - 1, corner(side, 0, 3)[t], 0.0)
            o = jnp.where(ok_y, o, 0.0)
            fy[side, t] = o
            value.append(o)
        add(5, [-2.0 * flat_2[t, along(near, k, y_half)] for t in two], value)

        for at in range(first, first + by, CHUNK):
            zero, one, two_e, two_i = (
                [field(t, layer, at, CHUNK) for t in two]
                for field, layer in ((f0, edge), (g1, edge), (g2, edge), (g2, inner)))
            one_i, two_t = ([field(t, layer, at, CHUNK) for t in two] for field, layer in ((g1, inner), (g2, third)))
            add(1, zero, one)
            add(2, one, one)
            for layer, f1_, f2_, next_ in ((edge, one, two_e, two_i), (inner, one_i, two_i, two_t)):
                add(3, f1_, f2_)
                add(4, f2_, f2_)
                left_a, left_b = rolled(f2_[0], 1), rolled(f2_[1], 1)
                z = (jnp.where(lane == 0, left_b, left_a), jnp.where(lane == 0, left_a, left_b))
                value = []
                for t in two:
                    other = z[t] + g2(t, layer, at - 1, CHUNK) + next_[t]
                    value.append(dd(t, layer, at, CHUNK) * f2_[t] - (other + other))
                add(5, f2_, value)

        parts = []
        more = corner(side, 0, 2)
        for at in range(0, x_half, CHUNK):
            begin = first + side * x_half + at
            f1h = [g1(t, halo, begin, CHUNK) for t in two]
            z = beside_z(*f1h)
            so_far = []
            for t in two:
                near_by = z[t] + g1(t, halo, begin - 1, CHUNK) + g1(t, halo, begin + 1, CHUNK)
                near_by = near_by + g1(t, edge, begin, CHUNK)
                so_far.append(near_by - jnp.where(row + begin == near, more[t], 0.0))
            parts.append((begin, f1h, so_far, [-2.0 * g2(t, edge, begin, CHUNK) for t in two]))

        @pl.when(ok)
        def _():
            some = xr.at[0, pl.ds(0, x_half * 3)]
            pltpu.make_async_copy(some, some, x_recv.at[2 + side]).wait()

        for n, (begin, f1h, so_far, weight) in enumerate(parts):
            shift, far = got(by * 3, x_half, n * CHUNK)
            value = [shift[t] * f1h[t] - so_far[t] - far[t] for t in two]
            value = [jnp.where(ok, v, 0.0) for v in (value[0], cut(value[1]))]
            for t in two:
                fx[side, t, pl.ds(begin - first, CHUNK)] = value[t]
            add(5, weight, value)
        return tuple(sums)

    sums[:] = lax.fori_loop(0, 2, x_phase, tuple(sums))

    while entered[0] <= len(stages):
        enter()
    lane_of = lane[:8]
    row_of = row[:8]
    stacked = zeros(8, LANES)
    for n, s in enumerate(sums):
        stacked = jnp.where(row_of == n, jnp.sum(s, 0, keepdims=True), stacked)
    packed = jnp.sum(jnp.where(lane_of == row_of, jnp.sum(stacked, 1, keepdims=True), 0.0), 0, keepdims=True)
    part[...] = packed

    @pl.loop(0, nx, unroll=nx * ny <= 64)
    def _(x):
        @pl.loop(0, ny, unroll=nx * ny <= 64)
        def _(y):
            @pl.when((x != gx) | (y != gy))
            def _():
                pltpu.make_async_remote_copy(
                    src_ref=part, dst_ref=slots.at[pl.ds(me, 1)], send_sem=sum_send.at[0],
                    recv_sem=sum_recv.at[0], device_id=(x, y), device_id_type=MESH).start()

    slots[pl.ds(me, 1)] = packed
    for d in two:
        _, edge, _ = x_side[1 - d]
        rows = pl.ds((1 - d) * x_half, x_half)
        start(lambda: [pltpu.make_async_remote_copy(
            src_ref=v2.at[:, edge, pl.ds(first + (1 - d) * x_half, x_half)], dst_ref=fx.at[d, :, rows],
            send_sem=fx_send.at[0], recv_sem=fx_recv.at[0],
            device_id=(gx + 1 - 2 * d, gy), device_id_type=MESH)], x_ok[1 - d])
        _, edge, _ = y_side[1 - d]
        for t in two:
            fys[d, t] = flat_2[t, along(edge, (1 - d) * y_half, y_half)]
        start(lambda: [pltpu.make_async_remote_copy(
            src_ref=fys.at[d], dst_ref=fyr.at[d], send_sem=fy_send.at[0], recv_sem=fy_recv.at[0],
            device_id=(gx, gy + 1 - 2 * d), device_id_type=MESH)], y_ok[1 - d])

    for k in range(bx):
        for at in range(first, first + by, CHUNK):
            out = apply(g2, k + 1, at, CHUNK, within(k))
            for t in two:
                v3[t, k, pl.ds(at - first, CHUNK)] = out[t]

    wait_all(xs, x_count, (1, 2), x_send)
    wait_all(ys, y_count, (1, 2), y_send)
    wait_all(cs, x_count * y_count, (1, 2, 4), c_send)
    half_x, half_y = fx.at[:, :, pl.ds(0, x_half)], fys
    wait_all(half_x, x_count, (1, 2), fx_send)
    wait_all(half_y, y_count, (1, 2), fy_send)
    others = slots.at[pl.ds(0, count - 1)]
    pltpu.make_async_copy(others, others, sum_send.at[0]).wait()
    wait_all(half_x, x_count, (1, 2), fx_recv)
    wait_all(half_y, y_count, (1, 2), fy_recv)
    for side in two:
        edge = x_side[side][1] - 1
        for t in two:
            v3[t, edge] = v3[t, edge] - fx[side, t]
        edge = y_side[side][1] - first
        for t in two:
            pieces = [fy[side, t], fyr[side, t]]
            rows = pl.ds(edge, bx, stride=by)
            flat_3[t, rows] = flat_3[t, rows] - jnp.concatenate(pieces[::-1] if side else pieces, 0)

    pltpu.make_async_copy(others, others, sum_recv.at[0]).wait()
    total = jnp.sum(slots[...], 0, keepdims=True)
    moment = [jnp.broadcast_to(total[:, k:k + 1], (1, LANES)) for k in range(6)]
    co = zeros(8, LANES)
    for k, c in enumerate(coefficients(moment)):
        co = jnp.where(row_of == k, c, co)
    co_ref[...] = co


def combine(f0m, f0t, v1, v2, v3, co_ref, x_out, r_out, x_buf, r_buf, sems):
    bx, by, bz = x_out.shape
    tail = bz - LANES
    c = [jnp.broadcast_to(co_ref[k:k + 1, :], (by, LANES)) for k in range(7)]
    rows = pl.ds(ROWS, by)

    def copy(n, k):
        src, dst = ((x_buf, x_out), (r_buf, r_out))[n]
        return pltpu.make_async_copy(src.at[pl.ds(k, 1)], dst.at[pl.ds(k, 1)], sems.at[n])

    for k in range(bx):
        for t in range(2):
            wide = LANES if t == 0 else tail
            lanes = slice(LANES * t, LANES * t + wide)
            f0 = f0t[k + 1, rows] if t else f0m[k + 1, rows]
            f1, f2, f3 = (v1[t, k + 1, rows], v2[t, k + 1, rows], v3[t, k])
            m = [a[:, :wide] for a in c]
            f1, f2, f3 = f1[:, :wide], f2[:, :wide], f3[:, :wide]
            x_buf[k, :, lanes] = m[0] * f0 + m[1] * f1 + m[2] * f2
            r_buf[k, :, lanes] = m[3] * f0 + m[4] * f1 + m[5] * f2 + m[6] * f3
        for n in range(2):
            copy(n, k).start()
    for n, (src, dst) in enumerate(((x_buf, x_out), (r_buf, r_out))):
        pltpu.make_async_copy(src, dst, sems.at[n]).wait()


def on_device(nx, ny, right_side, diagonal):
    bx, by, bz = right_side.shape
    tail = bz - LANES
    f32 = jnp.float32
    block = jax.ShapeDtypeStruct((bx, by, bz), f32)
    high, deep = bx + 2, by + 3 * ROWS
    vmem = pl.BlockSpec(memory_space=pltpu.VMEM)
    dma = pltpu.SemaphoreType.DMA
    shape = lambda *dims: jax.ShapeDtypeStruct(dims, f32)
    space = lambda *dims: pltpu.VMEM(dims, f32)
    x_rows, y_rows = by * 9 // 2, bx * 9 // 2
    fields = pl.pallas_call(
        functools.partial(kernel, nx, ny),
        out_shape=(shape(high, deep, LANES), shape(high, deep, tail), shape(2, high, deep, LANES),
                   shape(2, high, deep, LANES), shape(2, bx, by, LANES), shape(8, LANES)),
        in_specs=[pl.BlockSpec(memory_space=pltpu.HBM)] * 2,
        out_specs=(vmem,) * 6,
        scratch_shapes=[
            space(high, deep, LANES), space(high, deep, tail),
            space(2, x_rows, LANES), space(2, x_rows + 16, LANES), space(2, y_rows, LANES), space(2, y_rows, LANES),
            space(4, 8, LANES),
            space(2, deep, LANES), space(2, 2, bx, LANES), space(2, 2, bx + 2, LANES),
            space(2, 2, by, LANES), space(2, 2, bx // 2, LANES),
            space(2, 2, bx // 2, LANES), space(2, 2, bx // 2, LANES),
            space(1, LANES), space(nx * ny, LANES),
            dma((PIECES,)), dma((1,)), dma((4,)), dma((1,)), dma((1,)), dma((1,)), *[dma((1,))] * 6,
            pltpu.SemaphoreType.REGULAR((len(relay_reaches(ny)),)),
        ],
        compiler_params=pltpu.CompilerParams(
            collective_id=0, has_side_effects=True, vmem_limit_bytes=32 * 2**20),
    )(*(pltpu.with_memory_space_constraint(a, pltpu.HBM) for a in (right_side, diagonal)))
    return pl.pallas_call(
        combine,
        out_shape=(block, block),
        in_specs=[vmem] * 6,
        out_specs=(pl.BlockSpec(memory_space=pl.ANY),) * 2,
        scratch_shapes=[space(bx, by, bz), space(bx, by, bz), dma((2,))],
        compiler_params=pltpu.CompilerParams(vmem_limit_bytes=24 * 2**20),
    )(*fields)


def solution(mesh):
    placed = (P("gx", "gy", None), P("gx", "gy", None))
    return jax.shard_map(
        functools.partial(on_device, mesh.shape["gx"], mesh.shape["gy"]),
        mesh=mesh,
        in_specs=placed,
        out_specs=placed,
        check_vma=False,
    )
```
